32 devices in a mesh: dp: 2 (over x), cp: 16 (over z, y, core).
Axes of the slice: x: 2, y: 2, z: 4, core: 2. Of those that a mesh axis runs over, the one named last changes fastest.
Arguments:
- hidden: bfloat16 [32768, 4096], P(('dp', 'cp')), parts along dimension 0
- w_q: bfloat16 [4096, 4, 128], replicated
- w_k: bfloat16 [4096, 1, 128], replicated
- w_v: bfloat16 [4096, 1, 128], replicated
- w_o: bfloat16 [4, 128, 4096], replicated
Outputs:
- output: bfloat16 [32768, 4096], P(('dp', 'cp')), parts along dimension 0
There are 2 independent parts. The reference program is written for one: setup_inputs(seed, part) draws one part's arguments, and reference() takes and returns one part's arrays. A program takes and returns all parts, laid end to end along the dimension named above; an argument that names none is the same for every part.
All inputs are finite; a program needn't handle non-finite values.
Results may differ from the reference program's by a relative error of at most 0.00408156.
Values are sent between devices in bfloat16 or wider.
A program may use at most 1 GiB of HBM per device.

```python
import jax
import jax.numpy as jnp
from jax import lax

CP_SIZE = 16
CHUNK = 512
MODEL_DIM = 4096
HEADS = 4
KV_HEADS = 1
HEAD_DIM = 128
WINDOW = 4096
ROPE_BASE = 10000


def setup_inputs(seed: int = 0, part: int = 0) -> dict:
    seq_len = 2 * CP_SIZE * CHUNK
    weight_keys = jax.random.split(jax.random.key(seed), 4)
    part_key = jax.random.fold_in(jax.random.key(seed + 1), part)
    noise_key, chunk_key = jax.random.split(part_key)
    token_noise = jax.random.normal(noise_key, (2 * CP_SIZE, CHUNK, MODEL_DIM), jnp.float32)
    chunk_means = jax.random.normal(chunk_key, (2 * CP_SIZE, 1, MODEL_DIM), jnp.float32)
    natural = 0.6 * token_noise + 0.8 * chunk_means
    stored = jnp.stack([natural[:CP_SIZE], natural[CP_SIZE:][::-1]], axis=1).reshape(seq_len, MODEL_DIM)
    in_scale = MODEL_DIM ** -0.5
    out_scale = (HEADS * HEAD_DIM) ** -0.5
    w_q = jax.random.normal(weight_keys[0], (MODEL_DIM, HEADS, HEAD_DIM), jnp.float32) * in_scale
    w_k = jax.random.normal(weight_keys[1], (MODEL_DIM, KV_HEADS, HEAD_DIM), jnp.float32) * in_scale
    w_v = jax.random.normal(weight_keys[2], (MODEL_DIM, KV_HEADS, HEAD_DIM), jnp.float32) * in_scale
    w_o = jax.random.normal(weight_keys[3], (HEADS, HEAD_DIM, MODEL_DIM), jnp.float32) * out_scale
    return {'hidden': stored.astype(jnp.bfloat16), 'w_q': w_q.astype(jnp.bfloat16), 'w_k': w_k.astype(jnp.bfloat16), 'w_v': w_v.astype(jnp.bfloat16), 'w_o': w_o.astype(jnp.bfloat16)}


def rotate(values, positions, factor):
    half_dim = values.shape[-1] // 2
    inv_freq = 1.0 / (ROPE_BASE ** (jnp.arange(half_dim, dtype=jnp.float32) * (2.0 / values.shape[-1])))
    angles = positions.astype(jnp.float32)[..., None, None] * inv_freq
    cos_part = jnp.cos(angles)
    sin_part = jnp.sin(angles)
    first_half = values[..., :half_dim].astype(jnp.float32)
    second_half = values[..., half_dim:].astype(jnp.float32)
    rotated = jnp.concatenate([first_half * cos_part - second_half * sin_part, second_half * cos_part + first_half * sin_part], axis=-1)
    return (rotated * factor).astype(jnp.bfloat16)


def to_natural(stored):
    blocks = stored.reshape((CP_SIZE, 2, CHUNK) + stored.shape[1:])
    return jnp.concatenate([blocks[:, 0], blocks[::-1, 1]], axis=0).reshape(stored.shape)


def to_stored(natural):
    blocks = natural.reshape((2 * CP_SIZE, CHUNK) + natural.shape[1:])
    return jnp.stack([blocks[:CP_SIZE], blocks[CP_SIZE:][::-1]], axis=1).reshape(natural.shape)


def reference(hidden, w_q, w_k, w_v, w_o):
    seq_len = hidden.shape[0]
    group_size = HEADS // KV_HEADS
    dev_ids = jnp.arange(CP_SIZE)[:, None]
    chunk_ids = jnp.concatenate([dev_ids, 2 * CP_SIZE - 1 - dev_ids], axis=1)
    positions = (chunk_ids[:, :, None] * CHUNK + jnp.arange(CHUNK)).reshape(seq_len)
    q_flat = jnp.dot(hidden, w_q.reshape(MODEL_DIM, HEADS * HEAD_DIM), preferred_element_type=jnp.float32).astype(jnp.bfloat16)
    k_flat = jnp.dot(hidden, w_k.reshape(MODEL_DIM, KV_HEADS * HEAD_DIM), preferred_element_type=jnp.float32).astype(jnp.bfloat16)
    v_flat = jnp.dot(hidden, w_v.reshape(MODEL_DIM, KV_HEADS * HEAD_DIM), preferred_element_type=jnp.float32).astype(jnp.bfloat16)
    q_nat = to_natural(rotate(q_flat.reshape(seq_len, HEADS, HEAD_DIM), positions, HEAD_DIM ** -0.5))
    k_nat = to_natural(rotate(k_flat.reshape(seq_len, KV_HEADS, HEAD_DIM), positions, 1.0))
    v_nat = to_natural(v_flat.reshape(seq_len, KV_HEADS, HEAD_DIM))
    block_rows = min(CHUNK, 128)
    key_span = WINDOW + block_rows
    pad_zeros = jnp.zeros((WINDOW, KV_HEADS, HEAD_DIM), jnp.bfloat16)
    k_pad = jnp.concatenate([pad_zeros, k_nat], axis=0)
    v_pad = jnp.concatenate([pad_zeros, v_nat], axis=0)

    def one_block(block_id):
        row_start = block_id * block_rows
        q_part = lax.dynamic_slice_in_dim(q_nat, row_start, block_rows, axis=0).reshape(block_rows, KV_HEADS, group_size, HEAD_DIM)
        k_part = lax.dynamic_slice_in_dim(k_pad, row_start, key_span, axis=0)
        v_part = lax.dynamic_slice_in_dim(v_pad, row_start, key_span, axis=0)
        q_pos = row_start + jnp.arange(block_rows)
        k_pos = row_start - WINDOW + jnp.arange(key_span)
        allowed = (k_pos[None, :] <= q_pos[:, None]) & (q_pos[:, None] - k_pos[None, :] < WINDOW) & (k_pos[None, :] >= 0)
        scores = jnp.einsum('qkgd,skd->kgqs', q_part.astype(jnp.float32), k_part.astype(jnp.float32))
        scores = jnp.where(allowed, scores, -jnp.inf)
        row_max = jnp.max(scores, axis=-1, keepdims=True)
        exp_scores = jnp.exp(scores - row_max)
        row_sum = jnp.sum(exp_scores, axis=-1)
        attn_out = jnp.einsum('kgqs,skd->qkgd', exp_scores.astype(jnp.bfloat16).astype(jnp.float32), v_part.astype(jnp.float32))
        attn_out = attn_out / jnp.transpose(row_sum, (2, 0, 1))[..., None]
        return attn_out.astype(jnp.bfloat16).reshape(block_rows, HEADS * HEAD_DIM)

    o_nat = lax.map(one_block, jnp.arange(seq_len // block_rows)).reshape(seq_len, HEADS * HEAD_DIM)
    o_stored = to_stored(o_nat)
    return jnp.dot(o_stored, w_o.reshape(HEADS * HEAD_DIM, MODEL_DIM), preferred_element_type=jnp.float32).astype(jnp.bfloat16)
```

```python
import functools
import heapq

import jax
import jax.numpy as jnp
import numpy as np
from jax import lax
from jax.experimental import pallas as pl
from jax.experimental.pallas import tpu as pltpu

CHUNK, DIM, HD, HEADS = 512, 4096, 128, 4
TILE = 256
NT = HEADS * CHUNK // TILE
SLOTS, AHEAD = 4, 2
ROPE_BASE = 10000.0

NDEV, NCH = 16, 32
OFFS = (None, 4, -4, 2, -2)

def own(me): return (me, 31 - me)
def dst(me, f): return (me ^ 1) if f == 0 else me + OFFS[f]

def needs(me):
    s = set()
    for q in own(me):
        s |= {g for g in range(max(0, q - 8), q)}
    return s - set(own(me))

def routes():
    fwd = [dict() for _ in range(NDEV)]
    def add(me, g, f):
        fwd[me].setdefault(g, []).append(f)
    for me in range(NDEV):
        y, core = (me // 2) % 2, me % 2
        L, H = own(me)
        if me + 4 < 16: add(me, L, 1)
        if y == 0: add(me, L, 3)
        if core == 0 or me >= 12: add(me, L, 0)
        if me >= 14: add(me, L, 4); add(me, L, 2)
        if me - 4 >= 0: add(me, H, 2)
        if y == 1: add(me, H, 4)
        if core == 1: add(me, H, 0)
        for d in (1, 2, 3, 4):
            g = me - 2 * d
            if g >= 0:
                if d in (1, 2) and me + 4 < 16: add(me, g, 1)
                if d == 2 and y == 1: add(me, g, 4)
                if d == 1 and me >= 14: add(me, g, 2)
                if d < 4 or core == 1: add(me, g, 0)
            if me + 2 * d < 16:
                h = 31 - (me + 2 * d)
                if d in (1, 2) and me - 4 >= 0: add(me, h, 2)
                if d == 2 and y == 0: add(me, h, 3)
                if d < 4 or core == 0: add(me, h, 0)
        if me in (12, 13): add(me, me + 2, 2); add(me, me + 2, 0)
        if me in (10, 11): add(me, me + 2, 0); add(me, me + 4, 0)
        if me in (8, 9): add(me, me + 6, 0)
    return fwd

def check(fwd):
    recv = [dict() for _ in range(NDEV)]
    for me in range(NDEV):
        for g, fl in fwd[me].items():
            for f in fl:
                d = dst(me, f)
                assert 0 <= d < 16 and d != me, (me, g, f)
                assert g not in recv[d], (me, g, f, d, recv[d].get(g))
                assert g not in own(d)
                recv[d][g] = me
    for me in range(NDEV):
        for g in fwd[me]: assert g in own(me) or g in recv[me], (me, g)
        assert needs(me) <= set(recv[me]), (me, needs(me) - set(recv[me]))
    return recv

KVT = (3.3, 4.5)
T0, DIAG, DT = 9.5, 1.0, 1.2
LINK, LAT, D2D = 2.85, 1.9, 1.6
KMAX = 3

def plan():
    fwd = routes(); recv = check(fwd)
    link_free = {}
    arr = [dict() for _ in range(NDEV)]
    def send(me, g, now):
        for f in fwd[me].get(g, ()):
            d = dst(me, f)
            if f == 0:
                arr[d][g] = now + D2D
            else:
                k = (me // 2, f)
                s = max(now, link_free.get(k, 0.0))
                link_free[k] = s + LINK
                arr[d][g] = s + LINK + LAT
    acts = [[] for _ in range(NDEV)]
    items = [[] for _ in range(NDEV)]
    held = [set(own(m)) for m in range(NDEV)]
    todo = []
    for me in range(NDEV):
        L, H = own(me)
        todo.append([(c, g) for c, q in enumerate((L, H)) for g in range(max(0, q - 7), q)])
    ev = []
    for me in range(NDEV):
        heapq.heappush(ev, (KVT[0], 0, me, 'L')); heapq.heappush(ev, (KVT[1], 1, me, 'H'))
        heapq.heappush(ev, (T0, 2, me, 0))
    end = [0.0] * NDEV
    stall = [0.0] * NDEV
    nitem = [len(t) for t in todo]
    while ev:
        now, pr, me, what = heapq.heappop(ev)
        if what == 'L': send(me, own(me)[0], now); continue
        if what == 'H': send(me, own(me)[1], now); continue
        pos = what
        waited = []
        ready = sorted((t, g) for g, t in arr[me].items() if t <= now and g not in held[me])
        prio = sorted(ready, key=lambda tg: (-sum(1 for f in fwd[me].get(tg[1], ()) if f), tg[0]))
        for t, g in prio[:KMAX]:
            waited.append(g); held[me].add(g)
        last = pos == 3 + nitem[me]
        if 2 <= pos <= 2 + nitem[me] - 1 :
            def avail(): return [it for it in todo[me] if it[1] in held[me]]
            if not avail():
                cand = [(arr[me][g], g) for (c, g) in todo[me] if g in arr[me]]
                if not cand:
                    heapq.heappush(ev, (now + 0.1, 2, me, pos))
                    for g in waited: held[me].discard(g)
                    continue
                t, g = min(cand)
                if t > now:
                    for w in waited: held[me].discard(w)
                    stall[me] += t - now
                    heapq.heappush(ev, (t, 2, me, pos)); continue
                waited[-1:] = [g] if len(waited) == KMAX else waited[-1:] + [g]
                held[me] = (held[me] & (set(own(me)) | set(x for p in acts[me] for x in p))) | set(waited)
            it = avail()[0]
            lows = [i for i in avail() if i[0] == 0]; highs = [i for i in avail() if i[0] == 1]
            rem = {c: sum(1 for i in todo[me] if i[0] == c) for c in (0, 1)}
            pick = lows if (lows and (not highs or rem[0] >= rem[1])) else highs
            it = pick[0]
            todo[me].remove(it); items[me].append(it)
        if last:
            missing = [g for g in recv[me] if g not in held[me]]
            un = [arr[me].get(g) for g in missing]
            if any(t is None for t in un):
                for g in waited: held[me].discard(g)
                heapq.heappush(ev, (now + 0.1, 2, me, pos)); continue
            t = max([now] + un)
            if t > now:
                for g in waited: held[me].discard(g)
                stall[me] += t - now
                heapq.heappush(ev, (t, 2, me, pos)); continue
            waited += missing; held[me] |= set(missing)
            acts[me].append(waited)
            for g in waited: send(me, g, now)
            end[me] = now
            continue
        acts[me].append(waited)
        for g in waited: send(me, g, now)
        nxt = now + (DIAG if pos < 2 else (0.3 if pos == 2 else DT))
        heapq.heappush(ev, (nxt, 2, me, pos + 1))
    return fwd, recv, acts, items, nitem, end, stall, arr


def encode():
    fwd, recv, acts, items, nitem, _, _, _ = plan()
    code = lambda me, g: g + 32 * sum(1 << f for f in fwd[me].get(g, ()))
    npos = max(nitem) + 4
    act = [[-1] * NDEV for _ in range(npos * KMAX)]
    for me in range(NDEV):
        for p, gs in enumerate(acts[me]):
            assert len(gs) <= KMAX
            for k, g in enumerate(gs):
                act[p * KMAX + k][me] = code(me, g)
    item = [[(items[me][w][0] * 32 + items[me][w][1]) if w < nitem[me] else 0 for me in range(NDEV)] for w in range(max(nitem))]
    firsts = [[code(me, own(me)[c]) for me in range(NDEV)] for c in (0, 1)]
    return act, item, firsts, npos


ACT, ITEM, FIRST, NPOS = encode()
NITEM = len(ITEM)


def pick(me, row):
    common = max(set(row), key=lambda v: (row.count(v), v))
    out = jnp.int32(common)
    for i, v in enumerate(row):
        if v != common:
            out = jnp.where(me == i, jnp.int32(v), out)
    return out


def entry(values, at):
    if isinstance(at, int):
        return values[at]
    out = values[-1]
    for i, v in enumerate(values[:-1]):
        out = jnp.where(at == i, v, out)
    return out


def rope_tables():
    half = HD // 2
    freq = (np.float32(1.0) / np.power(np.float32(ROPE_BASE), np.arange(half, dtype=np.float32) * np.float32(2.0 / HD))).astype(np.float64)
    sign = np.concatenate([-np.ones(half), np.ones(half)])
    freq = np.concatenate([freq, freq])
    row = np.arange(CHUNK)[:, None] * freq
    base = (np.arange(NCH) * CHUNK)[:, None] * freq
    tabs = np.cos(row), np.sin(row) * sign, np.cos(base), np.sin(base) * sign
    return [t.astype(np.float32) for t in tabs]


def kernel(x_hbm, wq_hbm, wk_hbm, wv_hbm, cr_hbm, sr_hbm, cg_hbm, sg_hbm, o_ref,
           x, wq3, wq, wk, wv, cr, sr, cg, sg, cos, sin, kv, q, s_scr, p_scr, mx_scr, al_scr, m_ref, l_ref, acc,
           in_sem, send_sem, recv_sem):
    me = lax.axis_index('cp')
    core = lax.rem(me, 2)
    y = lax.rem(lax.div(me, 2), 2)

    loads = [(wk_hbm, wk), (wv_hbm, wv)]
    loads += [(x_hbm.at[pl.ds(i * TILE, TILE)], x.at[pl.ds(i * TILE, TILE)]) for i in range(2)]
    loads += [(cr_hbm, cr), (sr_hbm, sr), (cg_hbm, cg), (sg_hbm, sg)]
    loads += [(x_hbm.at[pl.ds(i * TILE, TILE)], x.at[pl.ds(i * TILE, TILE)]) for i in range(2, 4)]
    loads += [(wq_hbm, wq3)]
    loads = [pltpu.make_async_copy(a, b, in_sem.at[i]) for i, (a, b) in enumerate(loads)]
    for cp in loads:
        cp.start()

    sib = me + 1 - 2 * core
    mate = me + 2 - 4 * y
    bar = pltpu.get_barrier_semaphore()
    pl.semaphore_signal(bar, inc=1, device_id={'cp': sib}, device_id_type=pl.DeviceIdType.MESH)
    pl.semaphore_signal(bar, inc=1, device_id={'cp': mate}, device_id_type=pl.DeviceIdType.MESH)

    @pl.when(me + 4 < NDEV)
    def _():
        pl.semaphore_signal(bar, inc=1, device_id={'cp': me + 4}, device_id_type=pl.DeviceIdType.MESH)

    @pl.when(me >= 4)
    def _():
        pl.semaphore_signal(bar, inc=1, device_id={'cp': me - 4}, device_id_type=pl.DeviceIdType.MESH)

    acts = [[pick(me, ACT[p * KMAX + k]) for p in range(NPOS)] for k in range(KMAX)]
    item = [pick(me, row) for row in ITEM]

    def copy_to(g, f):
        to = (sib, me + 4, me - 4, me + 2, me - 2)[f]
        return pltpu.make_async_remote_copy(
            src_ref=kv.at[g], dst_ref=kv.at[g], send_sem=send_sem.at[f, g], recv_sem=recv_sem.at[g],
            device_id={'cp': to}, device_id_type=pl.DeviceIdType.MESH)

    def each_flag(code, do):
        g, flags = lax.rem(code, 32), lax.div(code, 32)
        for f in range(5):
            @pl.when(lax.rem(lax.div(flags, 1 << f), 2) == 1)
            def _():
                do(g, f)

    def send_on(code):
        each_flag(code, lambda g, f: copy_to(g, f).start())

    def drain(code):
        each_flag(code, lambda g, f: copy_to(g, f).wait_send())

    def actions(pos):
        for k in range(KMAX):
            code = entry(acts[k], pos)

            @pl.when(code >= 0)
            def _():
                copy_to(lax.rem(code, 32), 0).wait_recv()
                send_on(code)

    def own_chunk(c):
        return me + c * (NCH - 1 - 2 * me)

    def rope(v, c, rows):
        v = v.astype(jnp.bfloat16).astype(jnp.float32)
        return v * cos[c, rows] + pltpu.roll(v, HD // 2, 1) * sin[c, rows]

    loads[0].wait()
    loads[1].wait()
    wkv = jnp.concatenate([wk[...], wv[...]], axis=1)
    for c in range(2):
        g = own_chunk(c)
        if c == 0:
            for i in range(4, 8):
                loads[i].wait()
        cgr, sgr = cg[pl.ds(g, 1), :], sg[pl.ds(g, 1), :]
        cos[c] = cgr * cr[...] - sgr * sr[...]
        sin[c] = sgr * cr[...] + cgr * sr[...]
        for r in range(2):
            rows = slice(r * TILE, (r + 1) * TILE)
            loads[(2 + r) if c == 0 else (8 + r)].wait()
            both = jnp.dot(x[pl.ds(c * CHUNK + r * TILE, TILE), :], wkv, preferred_element_type=jnp.float32)
            kv[g, pl.ds(r * TILE, TILE), :] = rope(both[:, :HD], c, rows).astype(jnp.bfloat16)
            for b in range(2):
                vt = both[b * HD:(b + 1) * HD, HD:].T
                kv[g, pl.ds(CHUNK + (2 * r + b) * HD, HD), :] = vt.astype(jnp.bfloat16)
        if c == 0:
            pl.semaphore_wait(bar, 2 + jnp.where(me + 4 < NDEV, 1, 0) + jnp.where(me >= 4, 1, 0))
        send_on(pick(me, FIRST[c]))

    loads[10].wait()

    @pl.loop(0, DIM // TILE)
    def _(i):
        rows = pl.ds(pl.multiple_of(i * TILE, TILE), TILE)
        w = jnp.swapaxes(wq3[rows].astype(jnp.float32), 0, 1)
        for h in range(HEADS):
            wq[rows, pl.ds(h * HD, HD)] = w[h].astype(jnp.bfloat16)

    @pl.loop(0, 4)
    def _(i):
        c, r = lax.div(i, 2), lax.rem(i, 2)
        rows = pl.ds(pl.multiple_of(i * TILE, TILE), TILE)
        in_chunk = pl.ds(pl.multiple_of(r * TILE, TILE), TILE)
        qs = jnp.dot(x[rows, :], wq[...], preferred_element_type=jnp.float32)
        for h in range(HEADS):
            rot = rope(qs[:, h * HD:(h + 1) * HD], c, in_chunk)
            q[c * NT + h * 2 + r] = (rot * np.float32(HD ** -0.5)).astype(jnp.bfloat16)

    def scores(c, g, t, slot, k0=0, kn=CHUNK, mask=None):
        s = lax.dot_general(kv[g, pl.ds(k0, kn), :], q[c * NT + t], (((1,), (1,)), ((), ())), preferred_element_type=jnp.float32)
        if mask is not None:
            s = jnp.where(mask, s, -jnp.inf)
        s_scr[slot, pl.ds(0, kn), :] = s
        mx_scr[slot] = jnp.max(s.reshape(kn // 8, 8, TILE), axis=0)

    def softmax(c, t, slot, kn=CHUNK, first=False):
        n = c * NT + t
        mx = jnp.max(mx_scr[slot], axis=0, keepdims=True)
        if first:
            m_new = mx
        else:
            m_prev = m_ref[n]
            m_new = jnp.maximum(m_prev, mx)
            alpha = jnp.exp(m_prev - m_new)
            al_scr[slot] = alpha
        m_ref[n] = m_new
        p = jnp.exp(s_scr[slot, pl.ds(0, kn), :] - m_new)
        p_scr[slot, pl.ds(0, kn), :] = p.astype(jnp.bfloat16)
        part = jnp.sum(p.reshape(kn // 8, 8, TILE), axis=0)
        l_ref[n] = part if first else l_ref[n] * alpha + part

    def values(c, g, t, slot, k0=0, kn=CHUNK, first=False):
        vt = jnp.concatenate([kv[g, pl.ds(CHUNK + k0 + b, HD), :] for b in range(0, kn, HD)], axis=1)
        pv = jnp.dot(vt, p_scr[slot, pl.ds(0, kn), :], preferred_element_type=jnp.float32)
        n = c * NT + t
        acc[n] = pv if first else acc[n] * al_scr[slot] + pv

    key_i = lax.broadcasted_iota(jnp.int32, (CHUNK, TILE), 0)
    row_i = lax.broadcasted_iota(jnp.int32, (CHUNK, TILE), 1)

    def edge_block(c, g, far):
        def span(t):
            r = t % 2
            if far:
                return (0, CHUNK, key_i > row_i) if r == 0 else (TILE, TILE, key_i[:TILE] > row_i[:TILE])
            return (0, TILE, key_i[:TILE] <= row_i[:TILE]) if r == 0 else (0, CHUNK, key_i <= row_i + TILE)

        for t in range(NT + 2):
            if t < NT:
                scores(c, g, t, t % SLOTS, *span(t))
            if 1 <= t <= NT:
                softmax(c, t - 1, (t - 1) % SLOTS, span(t - 1)[1], first=not far)
            if t >= 2:
                k0, kn, _ = span(t - 2)
                values(c, g, t - 2, (t - 2) % SLOTS, k0, kn, first=not far)

    @pl.loop(0, 2)
    def _(c):
        actions(c)
        edge_block(c, own_chunk(c), False)

    n_full = jnp.minimum(me, 7) + 7
    actions(2)

    def c_and_g(code):
        return lax.div(code, 32), lax.rem(code, 32)

    c0, g0 = c_and_g(item[0])
    for t in range(AHEAD):
        scores(c0, g0, t, t)
    p_scr[SLOTS - 1] = jnp.zeros(p_scr.shape[1:], jnp.bfloat16)
    al_scr[SLOTS - 1] = jnp.ones(al_scr.shape[1:], jnp.float32)

    def full_block(w, carry):
        before, now = carry
        actions(w + 3)
        after = jnp.where(w + 1 < n_full, entry(item, w + 1), now)
        c, g = c_and_g(now)
        cn, gn = c_and_g(after)
        cp, gp = c_and_g(before)
        for t in range(NT):
            a = t + AHEAD
            if a < NT:
                scores(c, g, a, a % SLOTS)
            else:
                scores(cn, gn, a - NT, a % SLOTS)
            if t == 0:
                values(cp, gp, NT - 1, SLOTS - 1)
            else:
                values(c, g, t - 1, (t - 1) % SLOTS)
            softmax(c, t, t % SLOTS)
        return now, after

    cl, gl = c_and_g(lax.fori_loop(0, n_full, full_block, (item[0], item[0]))[0])
    values(cl, gl, NT - 1, SLOTS - 1)
    actions(n_full + 3)

    @pl.loop(jnp.where(me < 8, 1, 0), 2)
    def _(c):
        edge_block(c, own_chunk(c) - 8, True)

    @pl.loop(0, 2)
    def _(c):
        for t in range(NT):
            h, r = t // 2, t % 2
            n = c * NT + t
            out = acc[n] / jnp.sum(l_ref[n], axis=0, keepdims=True)
            o_ref[pl.ds(pl.multiple_of(c * CHUNK + r * TILE, TILE), TILE), pl.ds(h * HD, HD)] = out.T.astype(jnp.bfloat16)

    for c in range(2):
        drain(pick(me, FIRST[c]))

    for k in range(KMAX):
        @pl.loop(0, NPOS)
        def _(i):
            code = entry(acts[k], i)

            @pl.when(code >= 0)
            def _():
                drain(code)


def attend(hidden, w_q, w_k, w_v):
    any_spec = pl.BlockSpec(memory_space=pl.ANY)
    f32, bf16 = jnp.float32, jnp.bfloat16
    return pl.pallas_call(
        kernel,
        out_shape=jax.ShapeDtypeStruct((2 * CHUNK, HEADS * HD), bf16),
        in_specs=[any_spec] * 8,
        out_specs=pl.BlockSpec(memory_space=pltpu.VMEM),
        scratch_shapes=[
            pltpu.VMEM((2 * CHUNK, DIM), bf16),
            pltpu.VMEM((DIM, HEADS, HD), bf16),
            pltpu.VMEM((DIM, HEADS * HD), bf16),
            pltpu.VMEM((DIM, HD), bf16),
            pltpu.VMEM((DIM, HD), bf16),
            pltpu.VMEM((CHUNK, HD), f32),
            pltpu.VMEM((CHUNK, HD), f32),
            pltpu.VMEM((NCH, HD), f32),
            pltpu.VMEM((NCH, HD), f32),
            pltpu.VMEM((2, CHUNK, HD), f32),
            pltpu.VMEM((2, CHUNK, HD), f32),
            pltpu.VMEM((NCH, 2 * CHUNK, HD), bf16),
            pltpu.VMEM((2 * NT, TILE, HD), bf16),
            pltpu.VMEM((SLOTS, CHUNK, TILE), f32),
            pltpu.VMEM((SLOTS, CHUNK, TILE), bf16),
            pltpu.VMEM((SLOTS, 8, TILE), f32),
            pltpu.VMEM((SLOTS, 1, TILE), f32),
            pltpu.VMEM((2 * NT, 1, TILE), f32),
            pltpu.VMEM((2 * NT, 8, TILE), f32),
            pltpu.VMEM((2 * NT, HD, TILE), f32),
            pltpu.SemaphoreType.DMA((11,)),
            pltpu.SemaphoreType.DMA((5, NCH)),
            pltpu.SemaphoreType.DMA((NCH,)),
        ],
        compiler_params=pltpu.CompilerParams(
            collective_id=0, has_side_effects=True, vmem_limit_bytes=56 << 20),
        cost_estimate=pl.CostEstimate(flops=15 * 10 ** 9, bytes_accessed=16 << 20, transcendentals=1 << 24),
    )(hidden, w_q, w_k.reshape(DIM, HD), w_v.reshape(DIM, HD), *rope_tables())


def solution(mesh):
    def device_step(hidden, w_q, w_k, w_v, w_o):
        heads = attend(hidden, w_q, w_k, w_v)
        return jnp.dot(heads, w_o.reshape(HEADS * HD, DIM), preferred_element_type=jnp.float32).astype(jnp.bfloat16)

    from jax.sharding import PartitionSpec as P
    return jax.shard_map(device_step, mesh=mesh, in_specs=(P(('dp', 'cp'), None), P(), P(), P(), P()), out_specs=P(('dp', 'cp'), None), check_vma=False)
```

```python
import functools
import heapq

import jax
import jax.numpy as jnp
import numpy as np
from jax import lax
from jax.experimental import pallas as pl
from jax.experimental.pallas import tpu as pltpu

CHUNK, DIM, HD, HEADS = 512, 4096, 128, 4
TILE = 256
NT = HEADS * CHUNK // TILE
SLOTS, AHEAD = 4, 2
ROPE_BASE = 10000.0

NDEV, NCH = 16, 32
OFFS = (None, 4, -4, 2, -2)

def own(me): return (me, 31 - me)
def dst(me, f): return (me ^ 1) if f == 0 else me + OFFS[f]

def needs(me):
    s = set()
    for q in own(me):
        s |= {g for g in range(max(0, q - 8), q)}
    return s - set(own(me))

ACROSS = (0, 96)


def routes(across=None):
    low3, high3 = across or ACROSS
    fwd = [dict() for _ in range(NDEV)]
    def add(me, g, f):
        fwd[me].setdefault(g, []).append(f)
    for me in range(NDEV):
        y, core = (me // 2) % 2, me % 2
        L, H = own(me)
        if me + 4 < 16: add(me, L, 1)
        if y == 0: add(me, L, 3)
        if core == 0 or me >= 12: add(me, L, 0)
        if me >= 14: add(me, L, 4); add(me, L, 2)
        if me - 4 >= 0: add(me, H, 2)
        if y == 1: add(me, H, 4)
        if core == 1: add(me, H, 0)
        for d in (1, 2, 3, 4):
            g = me - 2 * d
            if g >= 0:
                by_y = (low3 >> (g // 2)) & 1
                ys = (g // 2) % 2
                if me + 4 < 16 and (d == 2 or (d == 1 and not by_y)): add(me, g, 1)
                if d == 2 and y == 1: add(me, g, 4)
                if by_y and d == 2 and ys == 0: add(me, g, 3)
                if by_y and d == 4 and ys == 1: add(me, g, 4)
                if by_y and ys == 1 and d == 1 and me + 4 >= 12 and me + 6 > 15 and me + 4 < 16: add(me, g, 1)
                if d == 1 and me >= 14: add(me, g, 2)
                if d < 4 or core == 1: add(me, g, 0)
            if me + 2 * d < 16:
                s = me + 2 * d
                h = 31 - s
                by_y = (high3 >> (s // 2)) & 1
                ys = (s // 2) % 2
                if me - 4 >= 0 and (d == 2 or (d == 1 and not by_y)): add(me, h, 2)
                if d == 2 and y == 0: add(me, h, 3)
                if by_y and d == 2 and ys == 1: add(me, h, 4)
                if by_y and d == 4 and ys == 0: add(me, h, 3)
                if by_y and ys == 0 and d == 1 and me - 6 < 0 and me - 4 >= 0: add(me, h, 2)
                if d < 4 or core == 0: add(me, h, 0)
        if me in (12, 13): add(me, me + 2, 2); add(me, me + 2, 0)
        if me in (10, 11): add(me, me + 2, 0); add(me, me + 4, 0)
        if me in (8, 9): add(me, me + 6, 0)
    return fwd


def check(fwd):
    recv = [dict() for _ in range(NDEV)]
    for me in range(NDEV):
        for g, fl in fwd[me].items():
            for f in fl:
                d = dst(me, f)
                assert 0 <= d < 16 and d != me, (me, g, f)
                assert g not in recv[d], (me, g, f, d, recv[d].get(g))
                assert g not in own(d)
                recv[d][g] = me
    for me in range(NDEV):
        for g in fwd[me]: assert g in own(me) or g in recv[me], (me, g)
        assert needs(me) <= set(recv[me]), (me, needs(me) - set(recv[me]))
    return recv

KVT = (4.2, 5.6)
PRE = (9.6, 9.6, 12.2, 12.2, 14.4, 14.4)
DT = 1.22
LINK, LAT, D2D = 2.85, 1.9, 1.6
KMAX = 2


def plan(across=None):
    fwd = routes(across); recv = check(fwd)
    npre = len(PRE)
    link_free = {}
    arr = [dict() for _ in range(NDEV)]

    def depth(me, g):
        return max([0] + [(0.1 if f == 0 else 1) + depth(dst(me, f), g) for f in fwd[me].get(g, ())])

    def send(me, g, now):
        for f in fwd[me].get(g, ()):
            d = dst(me, f)
            if f == 0:
                arr[d][g] = now + D2D
            else:
                k = (me // 2, f)
                s = max(now, link_free.get(k, 0.0))
                link_free[k] = s + LINK
                arr[d][g] = s + LINK + LAT

    acts = [[] for _ in range(NDEV)]
    items = [[] for _ in range(NDEV)]
    held = [set(own(m)) for m in range(NDEV)]
    todo = []
    for me in range(NDEV):
        todo.append([(c, g) for c, q in enumerate(own(me)) for g in range(max(0, q - 7), q)])
    nitem = [len(t) for t in todo]
    ev = []
    for me in range(NDEV):
        heapq.heappush(ev, (KVT[0], -2, me, 0))
        heapq.heappush(ev, (KVT[1], -1, me, 1))
        heapq.heappush(ev, (PRE[0], 0, me, 0))
    end = [0.0] * NDEV
    stall = [0.0] * NDEV
    while ev:
        now, pos, me, what = heapq.heappop(ev)
        if pos < 0:
            send(me, own(me)[what], now)
            continue
        have = held[me]
        ready = [g for g, t in arr[me].items() if t <= now and g not in have]
        waited = sorted(ready, key=lambda g: (-depth(me, g), arr[me][g]))[:KMAX]
        last = pos == npre + nitem[me]
        again = None
        if last:
            missing = [g for g in recv[me] if g not in have]
            times = [arr[me].get(g) for g in missing]
            if any(t is None for t in times):
                again = now + 0.1
            elif max([now] + times) > now:
                again = max(times)
            else:
                waited = missing
                assert len(waited) <= KMAX
        elif pos >= npre - 1 and pos - npre + 1 < nitem[me]:
            ok = [it for it in todo[me] if it[1] in have or it[1] in waited]
            if not ok:
                cand = sorted((arr[me][g], g) for c, g in todo[me] if g in arr[me])
                if not cand:
                    again = now + 0.1
                elif cand[0][0] > now:
                    again = cand[0][0]
                else:
                    waited = waited[:KMAX - 1] + [cand[0][1]]
                    ok = [it for it in todo[me] if it[1] in waited]
            if ok:
                rem = [sum(1 for it in todo[me] if it[0] == c) for c in (0, 1)]
                lead = 0 if rem[0] >= rem[1] else 1
                item = sorted(ok, key=lambda it: it[0] != lead)[0]
                todo[me].remove(item)
                items[me].append(item)
        if again is not None:
            stall[me] += again - now
            heapq.heappush(ev, (again, pos, me, 0))
            continue
        acts[me].append(waited)
        have |= set(waited)
        for g in waited:
            send(me, g, now)
        if last:
            end[me] = now
            continue
        if pos + 1 < npre:
            nxt = max(now, PRE[pos + 1])
        else:
            nxt = now + (0.3 if pos + 1 == npre else DT)
        heapq.heappush(ev, (nxt, pos + 1, me, 0))
    return fwd, recv, acts, items, nitem, end, stall, arr


def encode():
    fwd, recv, acts, items, nitem, _, _, _ = plan()
    code = lambda me, g: g + 32 * sum(1 << f for f in fwd[me].get(g, ()))
    npos = max(nitem) + len(PRE) + 1
    act = [[0] * NDEV for _ in range(npos)]
    for me in range(NDEV):
        for p, gs in enumerate(acts[me]):
            assert len(gs) <= KMAX == 2
            act[p][me] = sum((code(me, g) + 1) << (11 * k) for k, g in enumerate(gs))
    item = [[(items[me][w][0] * 32 + items[me][w][1]) if w < nitem[me] else 0 for me in range(NDEV)] for w in range(max(nitem))]
    firsts = [[code(me, own(me)[c]) for me in range(NDEV)] for c in (0, 1)]
    sent = []
    for f in range(5):
        lists = [sorted(g for g, fl in fwd[me].items() if f in fl) for me in range(NDEV)]
        for i in range(max(map(len, lists))):
            sent.append((f, [l[i] if i < len(l) else -1 for l in lists]))
    return act, item, firsts, sent


ACT, ITEM, FIRST, SENT = encode()


def pick(me, row):
    common = max(set(row), key=lambda v: (row.count(v), v))
    out = jnp.int32(common)
    for i, v in enumerate(row):
        if v != common:
            out = jnp.where(me == i, jnp.int32(v), out)
    return out


def entry(values, at):
    if isinstance(at, int):
        return values[at]
    out = values[-1]
    for i, v in enumerate(values[:-1]):
        out = jnp.where(at == i, v, out)
    return out


def rope_tables():
    half = HD // 2
    freq = (np.float32(1.0) / np.power(np.float32(ROPE_BASE), np.arange(half, dtype=np.float32) * np.float32(2.0 / HD))).astype(np.float64)
    sign = np.concatenate([-np.ones(half), np.ones(half)])
    freq = np.concatenate([freq, freq])
    row = np.arange(CHUNK)[:, None] * freq
    base = (np.arange(NCH) * CHUNK)[:, None] * freq
    tabs = np.cos(row), np.sin(row) * sign, np.cos(base), np.sin(base) * sign
    return [t.astype(np.float32) for t in tabs]


def kernel(x_hbm, wq_hbm, wk_hbm, wv_hbm, cr_hbm, sr_hbm, cg_hbm, sg_hbm, o_ref,
           x, wq3, wq, wk, wv, cr, sr, cg, sg, cos, sin, kv, q, flat, s_scr, p_scr, mx_scr, al_scr, m_ref, l_ref, acc,
           in_sem, send_sem, recv_sem):
    me = lax.axis_index('cp')
    core = lax.rem(me, 2)
    y = lax.rem(lax.div(me, 2), 2)

    loads = [(wk_hbm, wk), (wv_hbm, wv), (cr_hbm, cr), (sr_hbm, sr), (cg_hbm, cg), (sg_hbm, sg), (wq_hbm, wq3)]
    loads = [pltpu.make_async_copy(a, b, in_sem.at[i]) for i, (a, b) in enumerate(loads)]

    def load_x(c):
        rows = pl.ds(pl.multiple_of(c * CHUNK, CHUNK), CHUNK)
        return pltpu.make_async_copy(x_hbm.at[rows], x.at[rows], in_sem.at[7 + c])

    for cp in loads[:2] + [load_x(0)] + loads[2:6] + [load_x(1)] + loads[6:]:
        cp.start()

    sib = me + 1 - 2 * core
    mate = me + 2 - 4 * y
    bar = pltpu.get_barrier_semaphore()
    pl.semaphore_signal(bar, inc=1, device_id={'cp': sib}, device_id_type=pl.DeviceIdType.MESH)
    pl.semaphore_signal(bar, inc=1, device_id={'cp': mate}, device_id_type=pl.DeviceIdType.MESH)

    @pl.when(me + 4 < NDEV)
    def _():
        pl.semaphore_signal(bar, inc=1, device_id={'cp': me + 4}, device_id_type=pl.DeviceIdType.MESH)

    @pl.when(me >= 4)
    def _():
        pl.semaphore_signal(bar, inc=1, device_id={'cp': me - 4}, device_id_type=pl.DeviceIdType.MESH)

    acts = [pick(me, row) for row in ACT]
    item = [pick(me, row) for row in ITEM]

    def copy_to(g, f):
        to = (sib, me + 4, me - 4, me + 2, me - 2)[f]
        return pltpu.make_async_remote_copy(
            src_ref=kv.at[g], dst_ref=kv.at[g], send_sem=send_sem.at[f, g], recv_sem=recv_sem.at[g],
            device_id={'cp': to}, device_id_type=pl.DeviceIdType.MESH)

    def send_on(code):
        g, flags = lax.rem(code, 32), lax.div(code, 32)
        for f in range(5):
            @pl.when(lax.rem(lax.div(flags, 1 << f), 2) == 1)
            def _():
                copy_to(g, f).start()

    def actions(pos):
        packed = entry(acts, pos)

        @pl.when(packed > 0)
        def _():
            for k in range(KMAX):
                code = lax.rem(lax.div(packed, 1 << (11 * k)), 1 << 11) - 1

                @pl.when(code >= 0)
                def _():
                    copy_to(lax.rem(code, 32), 0).wait_recv()
                    send_on(code)

    def own_chunk(c):
        return me + c * (NCH - 1 - 2 * me)

    def rope(v, c, rows):
        v = v.astype(jnp.bfloat16).astype(jnp.float32)
        return v * cos[c, rows] + pltpu.roll(v, HD // 2, 1) * sin[c, rows]

    for cp in loads[:6]:
        cp.wait()
    first = [pick(me, row) for row in FIRST]

    @pl.loop(0, 2)
    def _(c):
        g = own_chunk(c)
        cgr, sgr = cg[pl.ds(g, 1), :], sg[pl.ds(g, 1), :]
        cos[c] = cgr * cr[...] - sgr * sr[...]
        sin[c] = sgr * cr[...] + cgr * sr[...]
        load_x(c).wait()
        wkv = jnp.concatenate([wk[...], wv[...]], axis=1)
        both = jnp.dot(x[pl.ds(pl.multiple_of(c * CHUNK, CHUNK), CHUNK), :], wkv, preferred_element_type=jnp.float32)
        kv[g, pl.ds(0, CHUNK), :] = rope(both[:, :HD], c, slice(0, CHUNK)).astype(jnp.bfloat16)
        for b in range(0, CHUNK, HD):
            kv[g, pl.ds(CHUNK + b, HD), :] = both[b:b + HD, HD:].T.astype(jnp.bfloat16)

        @pl.when(c == 0)
        def _():
            pl.semaphore_wait(bar, 2 + jnp.where(me + 4 < NDEV, 1, 0) + jnp.where(me >= 4, 1, 0))

        send_on(jnp.where(c == 0, first[0], first[1]))

    loads[6].wait()

    @pl.loop(0, DIM // TILE)
    def _(i):
        flat[...] = wq3[pl.ds(pl.multiple_of(i * HEADS * TILE, HEADS * TILE), HEADS * TILE), :].astype(jnp.float32)
        rows = pl.ds(pl.multiple_of(i * TILE, TILE), TILE)
        for h in range(HEADS):
            wq[rows, pl.ds(h * HD, HD)] = flat[pl.ds(h, TILE, stride=HEADS), :].astype(jnp.bfloat16)

    @pl.loop(0, 2)
    def _(c):
        @pl.when(c == 1)
        def _():
            actions(0)
            actions(1)

        qs = jnp.dot(x[pl.ds(pl.multiple_of(c * CHUNK, CHUNK), CHUNK), :], wq[...], preferred_element_type=jnp.float32)
        for h in range(HEADS):
            for r in range(2):
                rows = slice(r * TILE, (r + 1) * TILE)
                rot = rope(qs[rows, h * HD:(h + 1) * HD], c, rows)
                q[c * NT + h * 2 + r] = (rot * np.float32(HD ** -0.5)).astype(jnp.bfloat16)

    def scores(c, g, t, slot, k0=0, kn=CHUNK, mask=None):
        s = lax.dot_general(kv[g, pl.ds(k0, kn), :], q[c * NT + t], (((1,), (1,)), ((), ())), preferred_element_type=jnp.float32)
        if mask is not None:
            s = jnp.where(mask, s, -jnp.inf)
        s_scr[slot, pl.ds(0, kn), :] = s
        mx_scr[slot] = jnp.max(s.reshape(kn // 8, 8, TILE), axis=0)

    def softmax(c, t, slot, kn=CHUNK, first=False):
        n = c * NT + t
        mx = jnp.max(mx_scr[slot], axis=0, keepdims=True)
        if first:
            m_new = mx
        else:
            m_prev = m_ref[n]
            m_new = jnp.maximum(m_prev, mx)
            alpha = jnp.exp(m_prev - m_new)
            al_scr[slot] = alpha
        m_ref[n] = m_new
        p = jnp.exp(s_scr[slot, pl.ds(0, kn), :] - m_new)
        p_scr[slot, pl.ds(0, kn), :] = p.astype(jnp.bfloat16)
        part = jnp.sum(p.reshape(kn // 8, 8, TILE), axis=0)
        l_ref[n] = part if first else l_ref[n] * alpha + part

    def values(c, g, t, slot, k0=0, kn=CHUNK, first=False):
        vt = jnp.concatenate([kv[g, pl.ds(CHUNK + k0 + b, HD), :] for b in range(0, kn, HD)], axis=1)
        pv = jnp.dot(vt, p_scr[slot, pl.ds(0, kn), :], preferred_element_type=jnp.float32)
        n = c * NT + t
        acc[n] = pv if first else acc[n] * al_scr[slot] + pv

    key_i = lax.broadcasted_iota(jnp.int32, (CHUNK, TILE), 0)
    row_i = lax.broadcasted_iota(jnp.int32, (CHUNK, TILE), 1)

    none = jnp.where(me < 8, CHUNK, 0)

    def edge_blocks(far):
        def span(i):
            r = i % 2
            if far:
                row = row_i + none if i < NT else row_i
                return (0, CHUNK, key_i > row) if r == 0 else (TILE, TILE, key_i[:TILE] > row[:TILE])
            return (0, TILE, key_i[:TILE] <= row_i[:TILE]) if r == 0 else (0, CHUNK, key_i <= row_i + TILE)

        chunk = [jnp.maximum(own_chunk(c) - 8, 0) if far else own_chunk(c) for c in range(2)]
        for i in range(2 * NT + 2):
            if i < 2 * NT:
                scores(i // NT, chunk[i // NT], i % NT, i % SLOTS, *span(i))
            if 1 <= i <= 2 * NT:
                j = i - 1
                softmax(j // NT, j % NT, j % SLOTS, span(j)[1], first=not far)
            if i >= 2:
                j = i - 2
                values(j // NT, chunk[j // NT], j % NT, j % SLOTS, *span(j)[:2], first=not far)

    actions(2)
    actions(3)
    edge_blocks(False)

    n_full = jnp.minimum(me, 7) + 7
    actions(4)
    actions(5)

    def c_and_g(code):
        return lax.div(code, 32), lax.rem(code, 32)

    c0, g0 = c_and_g(item[0])
    for t in range(AHEAD):
        scores(c0, g0, t, t)
    p_scr[SLOTS - 1] = jnp.zeros(p_scr.shape[1:], jnp.bfloat16)
    al_scr[SLOTS - 1] = jnp.ones(al_scr.shape[1:], jnp.float32)

    def full_block(w, carry):
        before, now = carry
        actions(w + len(PRE))
        after = jnp.where(w + 1 < n_full, entry(item, w + 1), now)
        c, g = c_and_g(now)
        cn, gn = c_and_g(after)
        cp, gp = c_and_g(before)
        for t in range(NT):
            a = t + AHEAD
            if a < NT:
                scores(c, g, a, a % SLOTS)
            else:
                scores(cn, gn, a - NT, a % SLOTS)
            if t == 0:
                values(cp, gp, NT - 1, SLOTS - 1)
            else:
                values(c, g, t - 1, (t - 1) % SLOTS)
            softmax(c, t, t % SLOTS)
        return now, after

    cl, gl = c_and_g(lax.fori_loop(0, n_full, full_block, (item[0], item[0]))[0])
    values(cl, gl, NT - 1, SLOTS - 1)
    actions(n_full + len(PRE))

    edge_blocks(True)

    @pl.loop(0, 2)
    def _(c):
        for t in range(NT):
            h, r = t // 2, t % 2
            n = c * NT + t
            out = acc[n] / jnp.sum(l_ref[n], axis=0, keepdims=True)
            o_ref[pl.ds(pl.multiple_of(c * CHUNK + r * TILE, TILE), TILE), pl.ds(h * HD, HD)] = out.T.astype(jnp.bfloat16)

    for f, row in SENT:
        g = pick(me, row)

        @pl.when(g >= 0)
        def _():
            copy_to(g, f).wait_send()


def attend(hidden, w_q, w_k, w_v):
    any_spec = pl.BlockSpec(memory_space=pl.ANY)
    f32, bf16 = jnp.float32, jnp.bfloat16
    return pl.pallas_call(
        kernel,
        out_shape=pltpu.VMEM((2 * CHUNK, HEADS * HD), bf16),
        in_specs=[any_spec] * 8,
        out_specs=pl.BlockSpec(memory_space=pltpu.VMEM),
        scratch_shapes=[
            pltpu.VMEM((2 * CHUNK, DIM), bf16),
            pltpu.VMEM((DIM * HEADS, HD), bf16),
            pltpu.VMEM((DIM, HEADS * HD), bf16),
            pltpu.VMEM((DIM, HD), bf16),
            pltpu.VMEM((DIM, HD), bf16),
            pltpu.VMEM((CHUNK, HD), f32),
            pltpu.VMEM((CHUNK, HD), f32),
            pltpu.VMEM((NCH, HD), f32),
            pltpu.VMEM((NCH, HD), f32),
            pltpu.VMEM((2, CHUNK, HD), f32),
            pltpu.VMEM((2, CHUNK, HD), f32),
            pltpu.VMEM((NCH, 2 * CHUNK, HD), bf16),
            pltpu.VMEM((2 * NT, TILE, HD), bf16),
            pltpu.VMEM((HEADS * TILE, HD), f32),
            pltpu.VMEM((SLOTS, CHUNK, TILE), f32),
            pltpu.VMEM((SLOTS, CHUNK, TILE), bf16),
            pltpu.VMEM((SLOTS, 8, TILE), f32),
            pltpu.VMEM((SLOTS, 1, TILE), f32),
            pltpu.VMEM((2 * NT, 1, TILE), f32),
            pltpu.VMEM((2 * NT, 8, TILE), f32),
            pltpu.VMEM((2 * NT, HD, TILE), f32),
            pltpu.SemaphoreType.DMA((9,)),
            pltpu.SemaphoreType.DMA((5, NCH)),
            pltpu.SemaphoreType.DMA((NCH,)),
        ],
        compiler_params=pltpu.CompilerParams(
            collective_id=0, has_side_effects=True, vmem_limit_bytes=56 << 20),
        cost_estimate=pl.CostEstimate(flops=15 * 10 ** 9, bytes_accessed=16 << 20, transcendentals=1 << 24),
    )(hidden, w_q.reshape(DIM * HEADS, HD), w_k.reshape(DIM, HD), w_v.reshape(DIM, HD), *rope_tables())


def project(heads, w_o):
    rows = 256

    def body(a, w, out):
        mine = pl.ds(pl.multiple_of(pl.program_id(0) * rows, rows), rows)
        out[...] = jnp.dot(a[mine, :], w[...], preferred_element_type=jnp.float32).astype(jnp.bfloat16)

    return pl.pallas_call(
        body,
        grid=(2 * CHUNK // rows,),
        out_shape=jax.ShapeDtypeStruct((2 * CHUNK, DIM), jnp.bfloat16),
        in_specs=[pl.BlockSpec(memory_space=pltpu.VMEM)] * 2,
        out_specs=pl.BlockSpec((rows, DIM), lambda i: (i, 0)),
        compiler_params=pltpu.CompilerParams(vmem_limit_bytes=32 << 20),
        cost_estimate=pl.CostEstimate(flops=4 * 2 ** 30, bytes_accessed=13 << 20, transcendentals=0),
    )(heads, pltpu.with_memory_space_constraint(w_o, pltpu.VMEM))


def solution(mesh):
    def device_step(hidden, w_q, w_k, w_v, w_o):
        heads = attend(hidden, w_q, w_k, w_v)
        return project(heads, w_o.reshape(HEADS * HD, DIM))

    from jax.sharding import PartitionSpec as P
    return jax.shard_map(device_step, mesh=mesh, in_specs=(P(('dp', 'cp'), None), P(), P(), P(), P()), out_specs=P(('dp', 'cp'), None), check_vma=False)
```

```python
import functools
import heapq

import jax
import jax.numpy as jnp
import numpy as np
from jax import lax
from jax.experimental import pallas as pl
from jax.experimental.pallas import tpu as pltpu

CHUNK, DIM, HD, HEADS = 512, 4096, 128, 4
TILE = 256
NT = HEADS * CHUNK // TILE
SLOTS, AHEAD = 4, 2
ROPE_BASE = 10000.0

NDEV, NCH = 16, 32
OFFS = (None, 4, -4, 2, -2)

def own(me): return (me, 31 - me)
def dst(me, f): return (me ^ 1) if f == 0 else me + OFFS[f]

def needs(me):
    s = set()
    for q in own(me):
        s |= {g for g in range(max(0, q - 8), q)}
    return s - set(own(me))

ACROSS = (6, 96)


def routes(across=None):
    low3, high3 = across or ACROSS
    fwd = [dict() for _ in range(NDEV)]
    def add(me, g, f):
        fwd[me].setdefault(g, []).append(f)
    for me in range(NDEV):
        y, core = (me // 2) % 2, me % 2
        L, H = own(me)
        if me + 4 < 16: add(me, L, 1)
        if y == 0: add(me, L, 3)
        if core == 0 or me >= 12: add(me, L, 0)
        if me >= 14: add(me, L, 4); add(me, L, 2)
        if me - 4 >= 0: add(me, H, 2)
        if y == 1: add(me, H, 4)
        if core == 1: add(me, H, 0)
        for d in (1, 2, 3, 4):
            g = me - 2 * d
            if g >= 0:
                by_y = (low3 >> (g // 2)) & 1
                ys = (g // 2) % 2
                if me + 4 < 16 and (d == 2 or (d == 1 and not by_y)): add(me, g, 1)
                if d == 2 and y == 1: add(me, g, 4)
                if by_y and d == 2 and ys == 0: add(me, g, 3)
                if by_y and d == 4 and ys == 1: add(me, g, 4)
                if by_y and ys == 1 and d == 1 and me + 4 >= 12 and me + 6 > 15 and me + 4 < 16: add(me, g, 1)
                if d == 1 and me >= 14: add(me, g, 2)
                if d < 4 or core == 1: add(me, g, 0)
            if me + 2 * d < 16:
                s = me + 2 * d
                h = 31 - s
                by_y = (high3 >> (s // 2)) & 1
                ys = (s // 2) % 2
                if me - 4 >= 0 and (d == 2 or (d == 1 and not by_y)): add(me, h, 2)
                if d == 2 and y == 0: add(me, h, 3)
                if by_y and d == 2 and ys == 1: add(me, h, 4)
                if by_y and d == 4 and ys == 0: add(me, h, 3)
                if by_y and ys == 0 and d == 1 and me - 6 < 0 and me - 4 >= 0: add(me, h, 2)
                if d < 4 or core == 0: add(me, h, 0)
        if me in (12, 13): add(me, me + 2, 2); add(me, me + 2, 0)
        if me in (10, 11): add(me, me + 2, 0); add(me, me + 4, 0)
        if me in (8, 9): add(me, me + 6, 0)
    return fwd


def check(fwd):
    recv = [dict() for _ in range(NDEV)]
    for me in range(NDEV):
        for g, fl in fwd[me].items():
            for f in fl:
                d = dst(me, f)
                assert 0 <= d < 16 and d != me, (me, g, f)
                assert g not in recv[d], (me, g, f, d, recv[d].get(g))
                assert g not in own(d)
                recv[d][g] = me
    for me in range(NDEV):
        for g in fwd[me]: assert g in own(me) or g in recv[me], (me, g)
        assert needs(me) <= set(recv[me]), (me, needs(me) - set(recv[me]))
    return recv


NP, KS = 2, 4
PRE = (9.6, 12.2, 14.4)
KVT, DT, ACT_T, LINK, LAT, D2D, MARGIN, STEP = (4.5, 6.0), 1.27, 0.03, 2.82, 1.9, 1.5, 0.3, 0.03


def plan():
    fwd = routes()
    recv = check(fwd)
    npre=len(PRE)
    dep={}
    def depth(me,g):
        k=(me,g)
        if k not in dep: dep[k]=max([0]+[(0.1 if f==0 else 1)+depth(dst(me,f),g) for f in fwd[me].get(g,())])
        return dep[k]
    need=[set() for _ in range(NDEV)]
    todo=[]
    for me in range(NDEV):
        todo.append([(c,g) for c,q in enumerate(own(me)) for g in range(max(0,q-7),q)])
    nitem=[len(t) for t in todo]
    acts=[[] for _ in range(NDEV)]; items=[[] for _ in range(NDEV)]
    held=[{(g,p) for g in own(m) for p in range(NP)} for m in range(NDEV)]
    arr=[dict() for _ in range(NDEV)]
    queue={}; pend=[]
    def send(me,g,p,now):
        for f in fwd[me].get(g,()):
            d=dst(me,f)
            if f==0: heapq.heappush(pend,(now+D2D,d,(g,p)))
            else: queue.setdefault((me//2,f),({0:[],1:[]}))[me%2].append([1.0/NP,d,(g,p)])
    started=[[False,False] for _ in range(NDEV)]
    clock=[PRE[0]]*NDEV; pos=[0]*NDEV; end=[None]*NDEV; stall=[0.0]*NDEV
    npiece=[len(recv[m])*NP for m in range(NDEV)]
    now=0.0
    while any(e is None for e in end):
        if now>90: return None
        while pend and pend[0][0]<=now:
            tt,d,k=heapq.heappop(pend); arr[d][k]=tt
        for me in range(NDEV):
            for c in (0,1):
                if not started[me][c] and now>=KVT[c]:
                    started[me][c]=True
                    for p in range(NP): send(me,own(me)[c],p,now)
            if end[me] is not None or now<clock[me]: continue
            p=pos[me]; h=held[me]
            last=p==npre+nitem[me]
            ready=[k for k,t in arr[me].items() if k not in h and t+MARGIN<=now]
            take=sorted(ready,key=lambda k:(-depth(me,k[0]),arr[me][k]))[:KS]
            if last:
                if len(h)-2*NP+len([k for k in arr[me] if k not in h])<npiece[me]: stall[me]+=STEP; continue
                take=[k for k in arr[me] if k not in h]
                if len(take)>KS: return None
            elif p>=npre-1 and p-npre+1<nitem[me]:
                def ok_items(t):
                    hh=h|set(t)
                    return [it for it in todo[me] if all((it[1],q) in hh for q in range(NP))]
                ok=ok_items(take)
                if not ok:
                    full=[it for it in todo[me] if all((it[1],q) in h or (it[1],q) in arr[me] for q in range(NP))]
                    if not full: stall[me]+=STEP; continue
                    g=min(full,key=lambda it:max(arr[me].get((it[1],q),0) for q in range(NP)))[1]
                    must=[(g,q) for q in range(NP) if (g,q) not in h]
                    take=(must+[k for k in take if k not in must])[:KS]
                    ok=ok_items(take)
                rem=[sum(1 for it in todo[me] if it[0]==c) for c in (0,1)]
                lead=0 if rem[0]>=rem[1] else 1
                it=sorted(ok,key=lambda it:it[0]!=lead)[0]
                todo[me].remove(it); items[me].append(it)
            acts[me].append(take)
            h|=set(take)
            for k in take: send(me,k[0],k[1],now)
            if last: end[me]=now; continue
            pos[me]+=1
            if p+1<npre: clock[me]=max(now,PRE[p+1])
            else: clock[me]=now+ACT_T*len(take)+(0.3 if p+1==npre else DT)
        for k,qs in queue.items():
            act=[q for q in qs.values() if q]
            for q in act:
                q[0][0]-=STEP/LINK/len(act)
                if q[0][0]<=1e-9:
                    heapq.heappush(pend,(now+LAT,q[0][1],q[0][2])); q.pop(0)
        now+=STEP
    return fwd,recv,acts,items,nitem,end,stall,arr

def encode():
    fwd, recv, acts, items, nitem, _, _, _ = plan()
    code = lambda me, g, p: g * NP + p + 64 * sum(1 << f for f in fwd[me].get(g, ()))
    npos = max(nitem) + len(PRE) + 1
    look = [[[0] * NDEV for _ in range(npos)] for _ in range(KS // 2)]
    for me in range(NDEV):
        for pos, ks in enumerate(acts[me]):
            assert len(ks) <= KS
            for k, (g, p) in enumerate(ks):
                look[k // 2][pos][me] += (code(me, g, p) + 1) << (12 * (k % 2))
    item = [[(items[me][w][0] * 32 + items[me][w][1]) if w < nitem[me] else 0 for me in range(NDEV)] for w in range(max(nitem))]
    firsts = [[code(me, own(me)[c], 0) for me in range(NDEV)] for c in (0, 1)]
    sent = []
    for f in range(5):
        lists = [sorted(g for g, fl in fwd[me].items() if f in fl) for me in range(NDEV)]
        for i in range(max(map(len, lists))):
            sent.append((f, [l[i] if i < len(l) else -1 for l in lists]))
    return look, item, firsts, sent


LOOK, ITEM, FIRST, SENT = encode()


def pick(me, row):
    common = max(set(row), key=lambda v: (row.count(v), v))
    out = jnp.int32(common)
    for i, v in enumerate(row):
        if v != common:
            out = jnp.where(me == i, jnp.int32(v), out)
    return out


def entry(values, at):
    if isinstance(at, int):
        return values[at]
    out = values[-1]
    for i, v in enumerate(values[:-1]):
        out = jnp.where(at == i, v, out)
    return out


def rope_tables():
    half = HD // 2
    freq = (np.float32(1.0) / np.power(np.float32(ROPE_BASE), np.arange(half, dtype=np.float32) * np.float32(2.0 / HD))).astype(np.float64)
    sign = np.concatenate([-np.ones(half), np.ones(half)])
    freq = np.concatenate([freq, freq])
    row = np.arange(CHUNK)[:, None] * freq
    base = (np.arange(NCH) * CHUNK)[:, None] * freq
    tabs = np.cos(row), np.sin(row) * sign, np.cos(base), np.sin(base) * sign
    return [t.astype(np.float32) for t in tabs]


def kernel(x_hbm, wq_hbm, wk_hbm, wv_hbm, cr_hbm, sr_hbm, cg_hbm, sg_hbm, o_ref,
           x, wq3, wq, wk, wv, cr, sr, cg, sg, cos, sin, kv, q, flat, s_scr, p_scr, mx_scr, al_scr, m_ref, l_ref, acc,
           in_sem, send_sem, recv_sem):
    me = lax.axis_index('cp')
    core = lax.rem(me, 2)
    y = lax.rem(lax.div(me, 2), 2)

    loads = [(wk_hbm, wk), (wv_hbm, wv), (cr_hbm, cr), (sr_hbm, sr), (cg_hbm, cg), (sg_hbm, sg), (wq_hbm, wq3)]
    loads = [pltpu.make_async_copy(a, b, in_sem.at[i]) for i, (a, b) in enumerate(loads)]

    def load_x(c):
        rows = pl.ds(pl.multiple_of(c * CHUNK, CHUNK), CHUNK)
        return pltpu.make_async_copy(x_hbm.at[rows], x.at[rows], in_sem.at[7 + c])

    for cp in loads[:2] + [load_x(0)] + loads[2:6] + [load_x(1)] + loads[6:]:
        cp.start()

    sib = me + 1 - 2 * core
    mate = me + 2 - 4 * y
    bar = pltpu.get_barrier_semaphore()
    pl.semaphore_signal(bar, inc=1, device_id={'cp': sib}, device_id_type=pl.DeviceIdType.MESH)
    pl.semaphore_signal(bar, inc=1, device_id={'cp': mate}, device_id_type=pl.DeviceIdType.MESH)

    @pl.when(me + 4 < NDEV)
    def _():
        pl.semaphore_signal(bar, inc=1, device_id={'cp': me + 4}, device_id_type=pl.DeviceIdType.MESH)

    @pl.when(me >= 4)
    def _():
        pl.semaphore_signal(bar, inc=1, device_id={'cp': me - 4}, device_id_type=pl.DeviceIdType.MESH)

    looks = [[pick(me, row) for row in word] for word in LOOK]
    item = [pick(me, row) for row in ITEM]

    def copy_to(piece, f):
        to = (sib, me + 4, me - 4, me + 2, me - 2)[f]
        g, p = lax.div(piece, NP), lax.rem(piece, NP)
        part = kv.at[g, pl.ds(pl.multiple_of(p * CHUNK, CHUNK), CHUNK)]
        return pltpu.make_async_remote_copy(
            src_ref=part, dst_ref=part, send_sem=send_sem.at[f, g], recv_sem=recv_sem.at[piece],
            device_id={'cp': to}, device_id_type=pl.DeviceIdType.MESH)

    def send_on(code, pieces=1):
        piece, flags = lax.rem(code, 64), lax.div(code, 64)
        for f in range(5):
            @pl.when(lax.rem(lax.div(flags, 1 << f), 2) == 1)
            def _():
                for p in range(pieces):
                    copy_to(piece + p, f).start()

    def actions(pos):
        for word in looks:
            packed = entry(word, pos)

            @pl.when(packed > 0)
            def _():
                for k in range(2):
                    code = lax.rem(lax.div(packed, 1 << (12 * k)), 1 << 12) - 1

                    @pl.when(code >= 0)
                    def _():
                        copy_to(lax.rem(code, 64), 0).wait_recv()
                        send_on(code)

    def own_chunk(c):
        return me + c * (NCH - 1 - 2 * me)

    def rope(v, c, rows):
        v = v.astype(jnp.bfloat16).astype(jnp.float32)
        return v * cos[c, rows] + pltpu.roll(v, HD // 2, 1) * sin[c, rows]

    for cp in loads[:6]:
        cp.wait()
    first = [pick(me, row) for row in FIRST]

    @pl.loop(0, 2)
    def _(c):
        g = own_chunk(c)
        cgr, sgr = cg[pl.ds(g, 1), :], sg[pl.ds(g, 1), :]
        cos[c] = cgr * cr[...] - sgr * sr[...]
        sin[c] = sgr * cr[...] + cgr * sr[...]
        load_x(c).wait()
        wkv = jnp.concatenate([wk[...], wv[...]], axis=1)
        both = jnp.dot(x[pl.ds(pl.multiple_of(c * CHUNK, CHUNK), CHUNK), :], wkv, preferred_element_type=jnp.float32)
        kv[g, pl.ds(0, CHUNK), :] = rope(both[:, :HD], c, slice(0, CHUNK)).astype(jnp.bfloat16)
        for b in range(0, CHUNK, HD):
            kv[g, pl.ds(CHUNK + b, HD), :] = both[b:b + HD, HD:].T.astype(jnp.bfloat16)

        @pl.when(c == 0)
        def _():
            pl.semaphore_wait(bar, 2 + jnp.where(me + 4 < NDEV, 1, 0) + jnp.where(me >= 4, 1, 0))

        send_on(jnp.where(c == 0, first[0], first[1]), NP)

    loads[6].wait()

    @pl.loop(0, DIM // TILE)
    def _(i):
        flat[...] = wq3[pl.ds(pl.multiple_of(i * HEADS * TILE, HEADS * TILE), HEADS * TILE), :].astype(jnp.float32)
        rows = pl.ds(pl.multiple_of(i * TILE, TILE), TILE)
        for h in range(HEADS):
            wq[rows, pl.ds(h * HD, HD)] = flat[pl.ds(h, TILE, stride=HEADS), :].astype(jnp.bfloat16)

    @pl.loop(0, 2)
    def _(c):
        @pl.when(c == 1)
        def _():
            actions(0)

        qs = jnp.dot(x[pl.ds(pl.multiple_of(c * CHUNK, CHUNK), CHUNK), :], wq[...], preferred_element_type=jnp.float32)
        for h in range(HEADS):
            for r in range(2):
                rows = slice(r * TILE, (r + 1) * TILE)
                rot = rope(qs[rows, h * HD:(h + 1) * HD], c, rows)
                q[c * NT + h * 2 + r] = (rot * np.float32(HD ** -0.5)).astype(jnp.bfloat16)

    def scores(c, g, t, slot, k0=0, kn=CHUNK, mask=None):
        s = lax.dot_general(kv[g, pl.ds(k0, kn), :], q[c * NT + t], (((1,), (1,)), ((), ())), preferred_element_type=jnp.float32)
        if mask is not None:
            s = jnp.where(mask, s, -jnp.inf)
        s_scr[slot, pl.ds(0, kn), :] = s
        mx_scr[slot] = jnp.max(s.reshape(kn // 8, 8, TILE), axis=0)

    def softmax(c, t, slot, kn=CHUNK, first=False):
        n = c * NT + t
        mx = jnp.max(mx_scr[slot], axis=0, keepdims=True)
        if first:
            m_new = mx
        else:
            m_prev = m_ref[n]
            m_new = jnp.maximum(m_prev, mx)
            alpha = jnp.exp(m_prev - m_new)
            al_scr[slot] = alpha
        m_ref[n] = m_new
        p = jnp.exp(s_scr[slot, pl.ds(0, kn), :] - m_new)
        p_scr[slot, pl.ds(0, kn), :] = p.astype(jnp.bfloat16)
        part = jnp.sum(p.reshape(kn // 8, 8, TILE), axis=0)
        l_ref[n] = part if first else l_ref[n] * alpha + part

    def values(c, g, t, slot, k0=0, kn=CHUNK, first=False):
        vt = jnp.concatenate([kv[g, pl.ds(CHUNK + k0 + b, HD), :] for b in range(0, kn, HD)], axis=1)
        pv = jnp.dot(vt, p_scr[slot, pl.ds(0, kn), :], preferred_element_type=jnp.float32)
        n = c * NT + t
        acc[n] = pv if first else acc[n] * al_scr[slot] + pv

    key_i = lax.broadcasted_iota(jnp.int32, (CHUNK, TILE), 0)
    row_i = lax.broadcasted_iota(jnp.int32, (CHUNK, TILE), 1)

    none = jnp.where(me < 8, CHUNK, 0)

    def edge_blocks(far):
        def span(i):
            r = i % 2
            if far:
                row = row_i + none if i < NT else row_i
                return (0, CHUNK, key_i > row) if r == 0 else (TILE, TILE, key_i[:TILE] > row[:TILE])
            return (0, TILE, key_i[:TILE] <= row_i[:TILE]) if r == 0 else (0, CHUNK, key_i <= row_i + TILE)

        chunk = [jnp.maximum(own_chunk(c) - 8, 0) if far else own_chunk(c) for c in range(2)]
        for i in range(2 * NT + 2):
            if i < 2 * NT:
                scores(i // NT, chunk[i // NT], i % NT, i % SLOTS, *span(i))
            if 1 <= i <= 2 * NT:
                j = i - 1
                softmax(j // NT, j % NT, j % SLOTS, span(j)[1], first=not far)
            if i >= 2:
                j = i - 2
                values(j // NT, chunk[j // NT], j % NT, j % SLOTS, *span(j)[:2], first=not far)

    actions(1)
    edge_blocks(False)

    n_full = jnp.minimum(me, 7) + 7
    actions(2)

    def c_and_g(code):
        return lax.div(code, 32), lax.rem(code, 32)

    c0, g0 = c_and_g(item[0])
    for t in range(AHEAD):
        scores(c0, g0, t, t)
    p_scr[SLOTS - 1] = jnp.zeros(p_scr.shape[1:], jnp.bfloat16)
    al_scr[SLOTS - 1] = jnp.ones(al_scr.shape[1:], jnp.float32)

    def full_block(w, carry):
        before, now = carry
        actions(w + len(PRE))
        after = jnp.where(w + 1 < n_full, entry(item, w + 1), now)
        c, g = c_and_g(now)
        cn, gn = c_and_g(after)
        cp, gp = c_and_g(before)
        for t in range(NT):
            a = t + AHEAD
            if a < NT:
                scores(c, g, a, a % SLOTS)
            else:
                scores(cn, gn, a - NT, a % SLOTS)
            if t == 0:
                values(cp, gp, NT - 1, SLOTS - 1)
            else:
                values(c, g, t - 1, (t - 1) % SLOTS)
            softmax(c, t, t % SLOTS)
        return now, after

    cl, gl = c_and_g(lax.fori_loop(0, n_full, full_block, (item[0], item[0]))[0])
    values(cl, gl, NT - 1, SLOTS - 1)
    actions(n_full + len(PRE))

    edge_blocks(True)

    @pl.loop(0, 2)
    def _(c):
        for t in range(NT):
            h, r = t // 2, t % 2
            n = c * NT + t
            out = acc[n] / jnp.sum(l_ref[n], axis=0, keepdims=True)
            o_ref[pl.ds(pl.multiple_of(c * CHUNK + r * TILE, TILE), TILE), pl.ds(h * HD, HD)] = out.T.astype(jnp.bfloat16)

    for f, row in SENT:
        g = pick(me, row)

        @pl.when(g >= 0)
        def _():
            pltpu.make_async_remote_copy(
                src_ref=kv.at[g], dst_ref=kv.at[g], send_sem=send_sem.at[f, g], recv_sem=recv_sem.at[g * NP],
                device_id={'cp': sib}, device_id_type=pl.DeviceIdType.MESH).wait_send()


def attend(hidden, w_q, w_k, w_v):
    any_spec = pl.BlockSpec(memory_space=pl.ANY)
    f32, bf16 = jnp.float32, jnp.bfloat16
    return pl.pallas_call(
        kernel,
        out_shape=pltpu.VMEM((2 * CHUNK, HEADS * HD), bf16),
        in_specs=[any_spec] * 8,
        out_specs=pl.BlockSpec(memory_space=pltpu.VMEM),
        scratch_shapes=[
            pltpu.VMEM((2 * CHUNK, DIM), bf16),
            pltpu.VMEM((DIM * HEADS, HD), bf16),
            pltpu.VMEM((DIM, HEADS * HD), bf16),
            pltpu.VMEM((DIM, HD), bf16),
            pltpu.VMEM((DIM, HD), bf16),
            pltpu.VMEM((CHUNK, HD), f32),
            pltpu.VMEM((CHUNK, HD), f32),
            pltpu.VMEM((NCH, HD), f32),
            pltpu.VMEM((NCH, HD), f32),
            pltpu.VMEM((2, CHUNK, HD), f32),
            pltpu.VMEM((2, CHUNK, HD), f32),
            pltpu.VMEM((NCH, 2 * CHUNK, HD), bf16),
            pltpu.VMEM((2 * NT, TILE, HD), bf16),
            pltpu.VMEM((HEADS * TILE, HD), f32),
            pltpu.VMEM((SLOTS, CHUNK, TILE), f32),
            pltpu.VMEM((SLOTS, CHUNK, TILE), bf16),
            pltpu.VMEM((SLOTS, 8, TILE), f32),
            pltpu.VMEM((SLOTS, 1, TILE), f32),
            pltpu.VMEM((2 * NT, 1, TILE), f32),
            pltpu.VMEM((2 * NT, 8, TILE), f32),
            pltpu.VMEM((2 * NT, HD, TILE), f32),
            pltpu.SemaphoreType.DMA((9,)),
            pltpu.SemaphoreType.DMA((5, NCH)),
            pltpu.SemaphoreType.DMA((NCH * NP,)),
        ],
        compiler_params=pltpu.CompilerParams(
            collective_id=0, has_side_effects=True, vmem_limit_bytes=56 << 20),
        cost_estimate=pl.CostEstimate(flops=15 * 10 ** 9, bytes_accessed=16 << 20, transcendentals=1 << 24),
    )(hidden, w_q.reshape(DIM * HEADS, HD), w_k.reshape(DIM, HD), w_v.reshape(DIM, HD), *rope_tables())


def project(heads, w_o):
    rows = 256

    def body(a, w, out):
        mine = pl.ds(pl.multiple_of(pl.program_id(0) * rows, rows), rows)
        out[...] = jnp.dot(a[mine, :], w[...], preferred_element_type=jnp.float32).astype(jnp.bfloat16)

    return pl.pallas_call(
        body,
        grid=(2 * CHUNK // rows,),
        out_shape=jax.ShapeDtypeStruct((2 * CHUNK, DIM), jnp.bfloat16),
        in_specs=[pl.BlockSpec(memory_space=pltpu.VMEM)] * 2,
        out_specs=pl.BlockSpec((rows, DIM), lambda i: (i, 0)),
        compiler_params=pltpu.CompilerParams(vmem_limit_bytes=32 << 20),
        cost_estimate=pl.CostEstimate(flops=4 * 2 ** 30, bytes_accessed=13 << 20, transcendentals=0),
    )(heads, pltpu.with_memory_space_constraint(w_o, pltpu.VMEM))


def solution(mesh):
    def device_step(hidden, w_q, w_k, w_v, w_o):
        heads = attend(hidden, w_q, w_k, w_v)
        return project(heads, w_o.reshape(HEADS * HD, DIM))

    from jax.sharding import PartitionSpec as P
    return jax.shard_map(device_step, mesh=mesh, in_specs=(P(('dp', 'cp'), None), P(), P(), P(), P()), out_specs=P(('dp', 'cp'), None), check_vma=False)
```

```python
import functools
import heapq

import jax
import jax.numpy as jnp
import numpy as np
from jax import lax
from jax.experimental import pallas as pl
from jax.experimental.pallas import tpu as pltpu

CHUNK, DIM, HD, HEADS = 512, 4096, 128, 4
TILE = 256
NT = HEADS * CHUNK // TILE
SLOTS, AHEAD = 4, 2
ROPE_BASE = 10000.0

NDEV, NCH = 16, 32
OFFS = (None, 4, -4, 2, -2)

def own(me): return (me, 31 - me)
def dst(me, f): return (me ^ 1) if f == 0 else me + OFFS[f]

def needs(me):
    s = set()
    for q in own(me):
        s |= {g for g in range(max(0, q - 8), q)}
    return s - set(own(me))

ACROSS = (6, 96)


def routes(across=None):
    low3, high3 = across or ACROSS
    fwd = [dict() for _ in range(NDEV)]
    def add(me, g, f):
        fwd[me].setdefault(g, []).append(f)
    for me in range(NDEV):
        y, core = (me // 2) % 2, me % 2
        L, H = own(me)
        if me + 4 < 16: add(me, L, 1)
        if y == 0: add(me, L, 3)
        if core == 0 or me >= 12: add(me, L, 0)
        if me >= 14: add(me, L, 4); add(me, L, 2)
        if me - 4 >= 0: add(me, H, 2)
        if y == 1: add(me, H, 4)
        if core == 1: add(me, H, 0)
        for d in (1, 2, 3, 4):
            g = me - 2 * d
            if g >= 0:
                by_y = (low3 >> (g // 2)) & 1
                ys = (g // 2) % 2
                if me + 4 < 16 and (d == 2 or (d == 1 and not by_y)): add(me, g, 1)
                if d == 2 and y == 1: add(me, g, 4)
                if by_y and d == 2 and ys == 0: add(me, g, 3)
                if by_y and d == 4 and ys == 1: add(me, g, 4)
                if by_y and ys == 1 and d == 1 and me + 4 >= 12 and me + 6 > 15 and me + 4 < 16: add(me, g, 1)
                if d == 1 and me >= 14: add(me, g, 2)
                if d < 4 or core == 1: add(me, g, 0)
            if me + 2 * d < 16:
                s = me + 2 * d
                h = 31 - s
                by_y = (high3 >> (s // 2)) & 1
                ys = (s // 2) % 2
                if me - 4 >= 0 and (d == 2 or (d == 1 and not by_y)): add(me, h, 2)
                if d == 2 and y == 0: add(me, h, 3)
                if by_y and d == 2 and ys == 1: add(me, h, 4)
                if by_y and d == 4 and ys == 0: add(me, h, 3)
                if by_y and ys == 0 and d == 1 and me - 6 < 0 and me - 4 >= 0: add(me, h, 2)
                if d < 4 or core == 0: add(me, h, 0)
        if me in (12, 13): add(me, me + 2, 2); add(me, me + 2, 0)
        if me in (10, 11): add(me, me + 2, 0); add(me, me + 4, 0)
        if me in (8, 9): add(me, me + 6, 0)
    return fwd


def check(fwd):
    recv = [dict() for _ in range(NDEV)]
    for me in range(NDEV):
        for g, fl in fwd[me].items():
            for f in fl:
                d = dst(me, f)
                assert 0 <= d < 16 and d != me, (me, g, f)
                assert g not in recv[d], (me, g, f, d, recv[d].get(g))
                assert g not in own(d)
                recv[d][g] = me
    for me in range(NDEV):
        for g in fwd[me]: assert g in own(me) or g in recv[me], (me, g)
        assert needs(me) <= set(recv[me]), (me, needs(me) - set(recv[me]))
    return recv


NP, KS = 2, 4
WHOLE = -1
PRE = (9.6, 12.2, 14.4)
KVT, DT, ACT_T, LINK, LAT, D2D, MARGIN, STEP = (4.5, 6.0), 1.27, 0.03, 2.82, 1.9, 1.5, 0.3, 0.03


def plan():
    fwd = routes()
    recv = check(fwd)
    npre=len(PRE)
    dep={}
    def depth(me,g):
        k=(me,g)
        if k not in dep: dep[k]=max([0]+[(0.1 if f==0 else 1)+depth(dst(me,f),g) for f in fwd[me].get(g,())])
        return dep[k]
    need=[set() for _ in range(NDEV)]
    todo=[]
    for me in range(NDEV):
        todo.append([(c,g) for c,q in enumerate(own(me)) for g in range(max(0,q-7),q)])
    nitem=[len(t) for t in todo]
    acts=[[] for _ in range(NDEV)]; items=[[] for _ in range(NDEV)]
    held=[{(g,p) for g in own(m) for p in range(NP)} for m in range(NDEV)]
    arr=[dict() for _ in range(NDEV)]
    queue={}; pend=[]
    def send(me,g,p,now):
        for f in fwd[me].get(g,()):
            d=dst(me,f)
            if f==0: heapq.heappush(pend,(now+D2D,d,(g,p)))
            else: queue.setdefault((me//2,f),({0:[],1:[]}))[me%2].append([1.0/NP,d,(g,p)])
    def spread(ks): return {(g,r) for g,q in ks for r in range(NP) if q==WHOLE or q==r}
    started=[[False,False] for _ in range(NDEV)]
    clock=[PRE[0]]*NDEV; pos=[0]*NDEV; end=[None]*NDEV; stall=[0.0]*NDEV
    npiece=[len(recv[m])*NP for m in range(NDEV)]
    now=0.0
    while any(e is None for e in end):
        if now>90: return None
        while pend and pend[0][0]<=now:
            tt,d,k=heapq.heappop(pend); arr[d][k]=tt
        for me in range(NDEV):
            for c in (0,1):
                if not started[me][c] and now>=KVT[c]:
                    started[me][c]=True
                    for p in range(NP): send(me,own(me)[c],p,now)
            if end[me] is not None or now<clock[me]: continue
            p=pos[me]; h=held[me]
            last=p==npre+nitem[me]
            def units(when):
                out=[]
                for g in {k[0] for k in arr[me] if k not in h}:
                    if any(f for f in fwd[me].get(g,())):
                        out+=[(arr[me][(g,q)],g,q) for q in range(NP) if (g,q) in arr[me] and (g,q) not in h and arr[me][(g,q)]<=when]
                    elif all((g,q) in arr[me] for q in range(NP)):
                        t=max(arr[me][(g,q)] for q in range(NP))
                        if t<=when: out.append((t,g,WHOLE))
                return out
            take=[(g,q) for t,g,q in sorted(units(now-MARGIN),key=lambda u:(-depth(me,u[1]),u[0],u[1],u[2]))[:KS]]
            if last:
                if len(h)-2*NP+len([k for k in arr[me] if k not in h])<npiece[me]: stall[me]+=STEP; continue
                take=[(g,q) for t,g,q in sorted(units(now))]
                if len(take)>KS: return None
            elif p>=npre-1 and p-npre+1<nitem[me]:
                def ok_items(t):
                    hh=h|spread(t)
                    return [it for it in todo[me] if all((it[1],q) in hh for q in range(NP))]
                ok=ok_items(take)
                if not ok:
                    full=[it for it in todo[me] if all((it[1],q) in h or (it[1],q) in arr[me] for q in range(NP))]
                    if not full: stall[me]+=STEP; continue
                    g=min(full,key=lambda it:max(arr[me].get((it[1],q),0) for q in range(NP)))[1]
                    must=[(g2,q) for t,g2,q in units(now) if g2==g]
                    take=(must+[k for k in take if k not in must])[:KS]
                    ok=ok_items(take)
                rem=[sum(1 for it in todo[me] if it[0]==c) for c in (0,1)]
                lead=0 if rem[0]>=rem[1] else 1
                it=sorted(ok,key=lambda it:it[0]!=lead)[0]
                todo[me].remove(it); items[me].append(it)
            acts[me].append(take)
            h|=spread(take)
            for g,q in sorted(spread(take)): send(me,g,q,now)
            if last: end[me]=now; continue
            pos[me]+=1
            if p+1<npre: clock[me]=max(now,PRE[p+1])
            else: clock[me]=now+ACT_T*len(take)+(0.3 if p+1==npre else DT)
        for k,qs in queue.items():
            act=[q for q in qs.values() if q]
            for q in act:
                q[0][0]-=STEP/LINK/len(act)
                if q[0][0]<=1e-9:
                    heapq.heappush(pend,(now+LAT,q[0][1],q[0][2])); q.pop(0)
        now+=STEP
    return fwd,recv,acts,items,nitem,end,stall,arr

def encode():
    fwd, recv, acts, items, nitem, _, _, _ = plan()
    code = lambda me, g, p: g * NP + (0 if p == WHOLE else p) + 64 * sum(1 << f for f in fwd[me].get(g, ())) + 2048 * (p == WHOLE)
    npos = max(nitem) + len(PRE) + 1
    look = [[[0] * NDEV for _ in range(npos)] for _ in range(KS // 2)]
    for me in range(NDEV):
        for pos, ks in enumerate(acts[me]):
            assert len(ks) <= KS
            for k, (g, p) in enumerate(ks):
                look[k // 2][pos][me] += (code(me, g, p) + 1) << (13 * (k % 2))
    item = [[(items[me][w][0] * 32 + items[me][w][1]) if w < nitem[me] else 0 for me in range(NDEV)] for w in range(max(nitem))]
    firsts = [[code(me, own(me)[c], 0) for me in range(NDEV)] for c in (0, 1)]
    sent = []
    for f in range(5):
        lists = [sorted(g for g, fl in fwd[me].items() if f in fl) for me in range(NDEV)]
        for i in range(max(map(len, lists))):
            sent.append((f, [l[i] if i < len(l) else -1 for l in lists]))
    return look, item, firsts, sent


LOOK, ITEM, FIRST, SENT = encode()


def pick(me, row):
    common = max(set(row), key=lambda v: (row.count(v), v))
    out = jnp.int32(common)
    for i, v in enumerate(row):
        if v != common:
            out = jnp.where(me == i, jnp.int32(v), out)
    return out


def entry(values, at):
    if isinstance(at, int):
        return values[at]
    out = values[-1]
    for i, v in enumerate(values[:-1]):
        out = jnp.where(at == i, v, out)
    return out


def rope_tables():
    half = HD // 2
    freq = (np.float32(1.0) / np.power(np.float32(ROPE_BASE), np.arange(half, dtype=np.float32) * np.float32(2.0 / HD))).astype(np.float64)
    sign = np.concatenate([-np.ones(half), np.ones(half)])
    freq = np.concatenate([freq, freq])
    row = np.arange(CHUNK)[:, None] * freq
    base = (np.arange(NCH) * CHUNK)[:, None] * freq
    tabs = np.cos(row), np.sin(row) * sign, np.cos(base), np.sin(base) * sign
    return [t.astype(np.float32) for t in tabs]


def kernel(x_hbm, wq_hbm, wk_hbm, wv_hbm, cr_hbm, sr_hbm, cg_hbm, sg_hbm, o_ref,
           x, wq3, wq, wk, wv, cr, sr, cg, sg, cos, sin, kv, q, flat, s_scr, p_scr, mx_scr, al_scr, m_ref, l_ref, acc, tri,
           in_sem, send_sem, recv_sem):
    me = lax.axis_index('cp')
    core = lax.rem(me, 2)
    y = lax.rem(lax.div(me, 2), 2)

    loads = [(wk_hbm, wk), (wv_hbm, wv), (cr_hbm, cr), (sr_hbm, sr), (cg_hbm, cg), (sg_hbm, sg), (wq_hbm, wq3)]
    loads = [pltpu.make_async_copy(a, b, in_sem.at[i]) for i, (a, b) in enumerate(loads)]

    def load_x(c):
        rows = pl.ds(pl.multiple_of(c * CHUNK, CHUNK), CHUNK)
        return pltpu.make_async_copy(x_hbm.at[rows], x.at[rows], in_sem.at[7 + c])

    for cp in loads[:2] + [load_x(0)] + loads[2:6] + [load_x(1)] + loads[6:]:
        cp.start()

    sib = me + 1 - 2 * core
    mate = me + 2 - 4 * y
    bar = pltpu.get_barrier_semaphore()
    pl.semaphore_signal(bar, inc=1, device_id={'cp': sib}, device_id_type=pl.DeviceIdType.MESH)
    pl.semaphore_signal(bar, inc=1, device_id={'cp': mate}, device_id_type=pl.DeviceIdType.MESH)

    @pl.when(me + 4 < NDEV)
    def _():
        pl.semaphore_signal(bar, inc=1, device_id={'cp': me + 4}, device_id_type=pl.DeviceIdType.MESH)

    @pl.when(me >= 4)
    def _():
        pl.semaphore_signal(bar, inc=1, device_id={'cp': me - 4}, device_id_type=pl.DeviceIdType.MESH)

    looks = [[pick(me, row) for row in word] for word in LOOK]
    item = [pick(me, row) for row in ITEM]
    first = [pick(me, row) for row in FIRST]
    sent = [(f, pick(me, row)) for f, row in SENT]

    def copy_to(piece, f):
        to = (sib, me + 4, me - 4, me + 2, me - 2)[f]
        g, p = lax.div(piece, NP), lax.rem(piece, NP)
        part = kv.at[g, pl.ds(pl.multiple_of(p * CHUNK, CHUNK), CHUNK)]
        return pltpu.make_async_remote_copy(
            src_ref=part, dst_ref=part, send_sem=send_sem.at[f, g], recv_sem=recv_sem.at[piece],
            device_id={'cp': to}, device_id_type=pl.DeviceIdType.MESH)

    def send_on(code, pieces=1):
        piece, flags = lax.rem(code, 64), lax.div(code, 64)
        for f in range(5):
            @pl.when(lax.rem(lax.div(flags, 1 << f), 2) == 1)
            def _():
                for p in range(pieces):
                    copy_to(piece + p, f).start()

    def actions(pos):
        for word in looks:
            packed = entry(word, pos)

            @pl.when(packed > 0)
            def _():
                for k in range(2):
                    code = lax.rem(lax.div(packed, 1 << (13 * k)), 1 << 13) - 1

                    @pl.when((code >= 0) & (code < 2048))
                    def _():
                        copy_to(lax.rem(code, 64), 0).wait_recv()
                        send_on(code)

                    @pl.when(code >= 2048)
                    def _():
                        piece = lax.rem(code, 64)
                        for p in range(NP):
                            copy_to(piece + p, 0).wait_recv()

                        @pl.when(lax.rem(lax.div(code, 64), 2) == 1)
                        def _():
                            for p in range(NP):
                                copy_to(piece + p, 0).start()

    def own_chunk(c):
        return me + c * (NCH - 1 - 2 * me)

    def rope(v, c, rows):
        v = v.astype(jnp.bfloat16).astype(jnp.float32)
        return v * cos[c, rows] + pltpu.roll(v, HD // 2, 1) * sin[c, rows]

    for cp in loads[:6]:
        cp.wait()
    @pl.loop(0, 2)
    def _(c):
        g = own_chunk(c)
        cgr, sgr = cg[pl.ds(g, 1), :], sg[pl.ds(g, 1), :]
        cos[c] = cgr * cr[...] - sgr * sr[...]
        sin[c] = sgr * cr[...] + cgr * sr[...]
        load_x(c).wait()
        wkv = jnp.concatenate([wk[...], wv[...]], axis=1)
        both = jnp.dot(x[pl.ds(pl.multiple_of(c * CHUNK, CHUNK), CHUNK), :], wkv, preferred_element_type=jnp.float32)
        kv[g, pl.ds(0, CHUNK), :] = rope(both[:, :HD], c, slice(0, CHUNK)).astype(jnp.bfloat16)
        for b in range(0, CHUNK, HD):
            kv[g, pl.ds(CHUNK + b, HD), :] = both[b:b + HD, HD:].T.astype(jnp.bfloat16)

        @pl.when(c == 0)
        def _():
            pl.semaphore_wait(bar, 2 + jnp.where(me + 4 < NDEV, 1, 0) + jnp.where(me >= 4, 1, 0))

        send_on(jnp.where(c == 0, first[0], first[1]), NP)

    loads[6].wait()

    @pl.loop(0, DIM // TILE)
    def _(i):
        flat[...] = wq3[pl.ds(pl.multiple_of(i * HEADS * TILE, HEADS * TILE), HEADS * TILE), :].astype(jnp.float32)
        rows = pl.ds(pl.multiple_of(i * TILE, TILE), TILE)
        for h in range(HEADS):
            wq[rows, pl.ds(h * HD, HD)] = flat[pl.ds(h, TILE, stride=HEADS), :].astype(jnp.bfloat16)

    for c in range(2):
        if c == 1:
            actions(0)
        qs = jnp.dot(x[pl.ds(c * CHUNK, CHUNK), :], wq[...], preferred_element_type=jnp.float32)
        for h in range(HEADS):
            for r in range(2):
                rows = slice(r * TILE, (r + 1) * TILE)
                rot = rope(qs[rows, h * HD:(h + 1) * HD], c, rows)
                q[c * NT + h * 2 + r] = (rot * np.float32(HD ** -0.5)).astype(jnp.bfloat16)

    def scores(c, g, t, slot, k0=0, kn=CHUNK, bias=()):
        s = lax.dot_general(kv[g, pl.ds(k0, kn), :], q[c * NT + t], (((1,), (1,)), ((), ())), preferred_element_type=jnp.float32)
        parts = [s] if not bias else [s[i * TILE:(i + 1) * TILE] + b if b is not None else s[i * TILE:(i + 1) * TILE] for i, b in enumerate(bias)]
        tops = []
        for i, part in enumerate(parts):
            rows = part.shape[0]
            s_scr[slot, pl.ds(i * TILE, rows), :] = part
            tops.append(jnp.max(part.reshape(rows // 8, 8, TILE), axis=0))
        mx_scr[slot] = functools.reduce(jnp.maximum, tops)

    def softmax(c, t, slot, kn=CHUNK, first=False):
        n = c * NT + t
        mx = jnp.max(mx_scr[slot], axis=0, keepdims=True)
        if first:
            m_new = mx
        else:
            m_prev = m_ref[n]
            m_new = jnp.maximum(m_prev, mx)
            alpha = jnp.exp(m_prev - m_new)
            al_scr[slot] = alpha
        m_ref[n] = m_new
        p = jnp.exp(s_scr[slot, pl.ds(0, kn), :] - m_new)
        p_scr[slot, pl.ds(0, kn), :] = p.astype(jnp.bfloat16)
        part = jnp.sum(p.reshape(kn // 8, 8, TILE), axis=0)
        l_ref[n] = part if first else l_ref[n] * alpha + part

    def values(c, g, t, slot, k0=0, kn=CHUNK, first=False):
        vt = jnp.concatenate([kv[g, pl.ds(CHUNK + k0 + b, HD), :] for b in range(0, kn, HD)], axis=1)
        pv = jnp.dot(vt, p_scr[slot, pl.ds(0, kn), :], preferred_element_type=jnp.float32)
        n = c * NT + t
        acc[n] = pv if first else acc[n] * al_scr[slot] + pv

    key_i = lax.broadcasted_iota(jnp.int32, (TILE, TILE), 0)
    row_i = lax.broadcasted_iota(jnp.int32, (TILE, TILE), 1)
    none = jnp.where(me < 8, TILE, 0)
    tri[0] = jnp.where(key_i <= row_i, 0.0, -jnp.inf)
    tri[1] = jnp.where(key_i > row_i, 0.0, -jnp.inf)
    tri[2] = jnp.where(key_i > row_i + none, 0.0, -jnp.inf)
    low_far = jnp.where(me < 8, jnp.float32(-jnp.inf), jnp.float32(0.0))

    def edge_blocks(far):
        def span(i):
            r, low = i % 2, i < NT
            if far:
                edge = tri[2] if low else tri[1]
                return (0, CHUNK, (edge, low_far if low else None)) if r == 0 else (TILE, TILE, (edge,))
            return (0, TILE, (tri[0],)) if r == 0 else (0, CHUNK, (None, tri[0]))

        chunk = [jnp.maximum(own_chunk(c) - 8, 0) if far else own_chunk(c) for c in range(2)]
        for i in range(2 * NT + AHEAD + 1):
            if i < 2 * NT:
                scores(i // NT, chunk[i // NT], i % NT, i % SLOTS, *span(i))
            j = i - AHEAD - 1
            if j >= 0:
                values(j // NT, chunk[j // NT], j % NT, j % SLOTS, *span(j)[:2], first=not far)
            j = i - AHEAD
            if 0 <= j < 2 * NT:
                softmax(j // NT, j % NT, j % SLOTS, span(j)[1], first=not far)

    actions(1)
    edge_blocks(False)

    n_full = jnp.minimum(me, 7) + 7
    actions(2)

    def c_and_g(code):
        return lax.div(code, 32), lax.rem(code, 32)

    c0, g0 = c_and_g(item[0])
    for t in range(AHEAD):
        scores(c0, g0, t, t)
    p_scr[SLOTS - 1] = jnp.zeros(p_scr.shape[1:], jnp.bfloat16)
    al_scr[SLOTS - 1] = jnp.ones(al_scr.shape[1:], jnp.float32)

    def full_block(w, carry):
        before, now = carry
        actions(w + len(PRE))
        after = jnp.where(w + 1 < n_full, entry(item, w + 1), now)
        c, g = c_and_g(now)
        cn, gn = c_and_g(after)
        cp, gp = c_and_g(before)
        for t in range(NT):
            a = t + AHEAD
            if a < NT:
                scores(c, g, a, a % SLOTS)
            else:
                scores(cn, gn, a - NT, a % SLOTS)
            if t == 0:
                values(cp, gp, NT - 1, SLOTS - 1)
            else:
                values(c, g, t - 1, (t - 1) % SLOTS)
            softmax(c, t, t % SLOTS)
        return now, after

    cl, gl = c_and_g(lax.fori_loop(0, n_full, full_block, (item[0], item[0]))[0])
    values(cl, gl, NT - 1, SLOTS - 1)
    actions(n_full + len(PRE))

    edge_blocks(True)

    @pl.loop(0, 2)
    def _(c):
        for t in range(NT):
            h, r = t // 2, t % 2
            n = c * NT + t
            out = acc[n] / jnp.sum(l_ref[n], axis=0, keepdims=True)
            o_ref[pl.ds(pl.multiple_of(c * CHUNK + r * TILE, TILE), TILE), pl.ds(h * HD, HD)] = out.T.astype(jnp.bfloat16)

    for f, g in sent:
        @pl.when(g >= 0)
        def _():
            pltpu.make_async_remote_copy(
                src_ref=kv.at[g], dst_ref=kv.at[g], send_sem=send_sem.at[f, g], recv_sem=recv_sem.at[g * NP],
                device_id={'cp': sib}, device_id_type=pl.DeviceIdType.MESH).wait_send()


def attend(hidden, w_q, w_k, w_v):
    any_spec = pl.BlockSpec(memory_space=pl.ANY)
    f32, bf16 = jnp.float32, jnp.bfloat16
    return pl.pallas_call(
        kernel,
        out_shape=pltpu.VMEM((2 * CHUNK, HEADS * HD), bf16),
        in_specs=[any_spec] * 8,
        out_specs=pl.BlockSpec(memory_space=pltpu.VMEM),
        scratch_shapes=[
            pltpu.VMEM((2 * CHUNK, DIM), bf16),
            pltpu.VMEM((DIM * HEADS, HD), bf16),
            pltpu.VMEM((DIM, HEADS * HD), bf16),
            pltpu.VMEM((DIM, HD), bf16),
            pltpu.VMEM((DIM, HD), bf16),
            pltpu.VMEM((CHUNK, HD), f32),
            pltpu.VMEM((CHUNK, HD), f32),
            pltpu.VMEM((NCH, HD), f32),
            pltpu.VMEM((NCH, HD), f32),
            pltpu.VMEM((2, CHUNK, HD), f32),
            pltpu.VMEM((2, CHUNK, HD), f32),
            pltpu.VMEM((NCH, 2 * CHUNK, HD), bf16),
            pltpu.VMEM((2 * NT, TILE, HD), bf16),
            pltpu.VMEM((HEADS * TILE, HD), f32),
            pltpu.VMEM((SLOTS, CHUNK, TILE), f32),
            pltpu.VMEM((SLOTS, CHUNK, TILE), bf16),
            pltpu.VMEM((SLOTS, 8, TILE), f32),
            pltpu.VMEM((SLOTS, 1, TILE), f32),
            pltpu.VMEM((2 * NT, 1, TILE), f32),
            pltpu.VMEM((2 * NT, 8, TILE), f32),
            pltpu.VMEM((2 * NT, HD, TILE), f32),
            pltpu.VMEM((3, TILE, TILE), f32),
            pltpu.SemaphoreType.DMA((9,)),
            pltpu.SemaphoreType.DMA((5, NCH)),
            pltpu.SemaphoreType.DMA((NCH * NP,)),
        ],
        compiler_params=pltpu.CompilerParams(
            collective_id=0, has_side_effects=True, vmem_limit_bytes=56 << 20),
        cost_estimate=pl.CostEstimate(flops=15 * 10 ** 9, bytes_accessed=16 << 20, transcendentals=1 << 24),
    )(hidden, w_q.reshape(DIM * HEADS, HD), w_k.reshape(DIM, HD), w_v.reshape(DIM, HD), *rope_tables())


def project(heads, w_o):
    rows = 256

    def body(a, w, out):
        mine = pl.ds(pl.multiple_of(pl.program_id(0) * rows, rows), rows)
        out[...] = jnp.dot(a[mine, :], w[...], preferred_element_type=jnp.float32).astype(jnp.bfloat16)

    return pl.pallas_call(
        body,
        grid=(2 * CHUNK // rows,),
        out_shape=jax.ShapeDtypeStruct((2 * CHUNK, DIM), jnp.bfloat16),
        in_specs=[pl.BlockSpec(memory_space=pltpu.VMEM)] * 2,
        out_specs=pl.BlockSpec((rows, DIM), lambda i: (i, 0)),
        compiler_params=pltpu.CompilerParams(vmem_limit_bytes=32 << 20),
        cost_estimate=pl.CostEstimate(flops=4 * 2 ** 30, bytes_accessed=13 << 20, transcendentals=0),
    )(heads, pltpu.with_memory_space_constraint(w_o, pltpu.VMEM))


def solution(mesh):
    def device_step(hidden, w_q, w_k, w_v, w_o):
        heads = attend(hidden, w_q, w_k, w_v)
        return project(heads, w_o.reshape(HEADS * HD, DIM))

    from jax.sharding import PartitionSpec as P
    return jax.shard_map(device_step, mesh=mesh, in_specs=(P(('dp', 'cp'), None), P(), P(), P(), P()), out_specs=P(('dp', 'cp'), None), check_vma=False)
```

```python
import functools
import heapq

import jax
import jax.numpy as jnp
import numpy as np
from jax import lax
from jax.experimental import pallas as pl
from jax.experimental.pallas import tpu as pltpu

CHUNK, DIM, HD, HEADS = 512, 4096, 128, 4
TILE = 256
NT = HEADS * CHUNK // TILE
SLOTS, AHEAD = 4, 2
ROPE_BASE = 10000.0

NDEV, NCH = 16, 32
OFFS = (None, 4, -4, 2, -2)

def own(me): return (me, 31 - me)
def dst(me, f): return (me ^ 1) if f == 0 else me + OFFS[f]

def needs(me):
    s = set()
    for q in own(me):
        s |= {g for g in range(max(0, q - 8), q)}
    return s - set(own(me))

ACROSS = (6, 96)


def routes(across=None):
    low3, high3 = across or ACROSS
    fwd = [dict() for _ in range(NDEV)]
    def add(me, g, f):
        fwd[me].setdefault(g, []).append(f)
    for me in range(NDEV):
        y, core = (me // 2) % 2, me % 2
        L, H = own(me)
        if me + 4 < 16: add(me, L, 1)
        if y == 0: add(me, L, 3)
        if core == 0 or me >= 12: add(me, L, 0)
        if me >= 14: add(me, L, 4); add(me, L, 2)
        if me - 4 >= 0: add(me, H, 2)
        if y == 1: add(me, H, 4)
        if core == 1: add(me, H, 0)
        for d in (1, 2, 3, 4):
            g = me - 2 * d
            if g >= 0:
                by_y = (low3 >> (g // 2)) & 1
                ys = (g // 2) % 2
                if me + 4 < 16 and (d == 2 or (d == 1 and not by_y)): add(me, g, 1)
                if d == 2 and y == 1: add(me, g, 4)
                if by_y and d == 2 and ys == 0: add(me, g, 3)
                if by_y and d == 4 and ys == 1: add(me, g, 4)
                if by_y and ys == 1 and d == 1 and me + 4 >= 12 and me + 6 > 15 and me + 4 < 16: add(me, g, 1)
                if d == 1 and me >= 14: add(me, g, 2)
                if d < 4 or core == 1: add(me, g, 0)
            if me + 2 * d < 16:
                s = me + 2 * d
                h = 31 - s
                by_y = (high3 >> (s // 2)) & 1
                ys = (s // 2) % 2
                if me - 4 >= 0 and (d == 2 or (d == 1 and not by_y)): add(me, h, 2)
                if d == 2 and y == 0: add(me, h, 3)
                if by_y and d == 2 and ys == 1: add(me, h, 4)
                if by_y and d == 4 and ys == 0: add(me, h, 3)
                if by_y and ys == 0 and d == 1 and me - 6 < 0 and me - 4 >= 0: add(me, h, 2)
                if d < 4 or core == 0: add(me, h, 0)
        if me in (12, 13): add(me, me + 2, 2); add(me, me + 2, 0)
        if me in (10, 11): add(me, me + 2, 0); add(me, me + 4, 0)
        if me in (8, 9): add(me, me + 6, 0)
    return fwd


def check(fwd):
    recv = [dict() for _ in range(NDEV)]
    for me in range(NDEV):
        for g, fl in fwd[me].items():
            for f in fl:
                d = dst(me, f)
                assert 0 <= d < 16 and d != me, (me, g, f)
                assert g not in recv[d], (me, g, f, d, recv[d].get(g))
                assert g not in own(d)
                recv[d][g] = me
    for me in range(NDEV):
        for g in fwd[me]: assert g in own(me) or g in recv[me], (me, g)
        assert needs(me) <= set(recv[me]), (me, needs(me) - set(recv[me]))
    return recv


NP, KS = 2, 4
WHOLE = -1
PRE = (9.3, 11.9, 14.0)
KVT, DT, ACT_T, LINK, LAT, D2D, MARGIN, STEP = (4.3, 5.8), 1.22, 0.05, 2.82, 1.9, 1.5, 0.3, 0.03


def plan():
    fwd = routes()
    recv = check(fwd)
    npre=len(PRE)
    dep={}
    def depth(me,g):
        k=(me,g)
        if k not in dep: dep[k]=max([0]+[(0.1 if f==0 else 1)+depth(dst(me,f),g) for f in fwd[me].get(g,())])
        return dep[k]
    need=[set() for _ in range(NDEV)]
    todo=[]
    for me in range(NDEV):
        todo.append([(c,g) for c,q in enumerate(own(me)) for g in range(max(0,q-7),q)])
    nitem=[len(t) for t in todo]
    acts=[[] for _ in range(NDEV)]; items=[[] for _ in range(NDEV)]
    held=[{(g,p) for g in own(m) for p in range(NP)} for m in range(NDEV)]
    arr=[dict() for _ in range(NDEV)]
    queue={}; pend=[]
    def send(me,g,p,now):
        for f in fwd[me].get(g,()):
            d=dst(me,f)
            if f==0: heapq.heappush(pend,(now+D2D,d,(g,p)))
            else: queue.setdefault((me//2,f),({0:[],1:[]}))[me%2].append([1.0/NP,d,(g,p)])
    def spread(ks): return {(g,r) for g,q in ks for r in range(NP) if q==WHOLE or q==r}
    started=[[False,False] for _ in range(NDEV)]
    clock=[PRE[0]]*NDEV; pos=[0]*NDEV; end=[None]*NDEV; stall=[0.0]*NDEV
    npiece=[len(recv[m])*NP for m in range(NDEV)]
    now=0.0
    while any(e is None for e in end):
        if now>90: return None
        while pend and pend[0][0]<=now:
            tt,d,k=heapq.heappop(pend); arr[d][k]=tt
        for me in range(NDEV):
            for c in (0,1):
                if not started[me][c] and now>=KVT[c]:
                    started[me][c]=True
                    for p in range(NP): send(me,own(me)[c],p,now)
            if end[me] is not None or now<clock[me]: continue
            p=pos[me]; h=held[me]
            last=p==npre+nitem[me]
            def units(when):
                out=[]
                for g in {k[0] for k in arr[me] if k not in h}:
                    if any(f for f in fwd[me].get(g,())):
                        out+=[(arr[me][(g,q)],g,q) for q in range(NP) if (g,q) in arr[me] and (g,q) not in h and arr[me][(g,q)]<=when]
                    elif all((g,q) in arr[me] for q in range(NP)):
                        t=max(arr[me][(g,q)] for q in range(NP))
                        if t<=when: out.append((t,g,WHOLE))
                return out
            take=[(g,q) for t,g,q in sorted(units(now-MARGIN),key=lambda u:(-depth(me,u[1]),u[0],u[1],u[2]))[:KS]]
            if last:
                if len(h)-2*NP+len([k for k in arr[me] if k not in h])<npiece[me]: stall[me]+=STEP; continue
                take=[(g,q) for t,g,q in sorted(units(now))]
                if len(take)>KS: return None
            elif p>=npre-1 and p-npre+1<nitem[me]:
                def ok_items(t):
                    hh=h|spread(t)
                    return [it for it in todo[me] if all((it[1],q) in hh for q in range(NP))]
                ok=ok_items(take)
                if not ok:
                    full=[it for it in todo[me] if all((it[1],q) in h or (it[1],q) in arr[me] for q in range(NP))]
                    if not full: stall[me]+=STEP; continue
                    g=min(full,key=lambda it:max(arr[me].get((it[1],q),0) for q in range(NP)))[1]
                    must=[(g2,q) for t,g2,q in units(now) if g2==g]
                    take=(must+[k for k in take if k not in must])[:KS]
                    ok=ok_items(take)
                rem=[sum(1 for it in todo[me] if it[0]==c) for c in (0,1)]
                lead=0 if rem[0]>=rem[1] else 1
                it=sorted(ok,key=lambda it:it[0]!=lead)[0]
                todo[me].remove(it); items[me].append(it)
            acts[me].append(take)
            h|=spread(take)
            for g,q in sorted(spread(take)): send(me,g,q,now)
            if last: end[me]=now; continue
            pos[me]+=1
            if p+1<npre: clock[me]=max(now,PRE[p+1])
            else: clock[me]=now+ACT_T*len(take)+(0.3 if p+1==npre else DT)
        for k,qs in queue.items():
            act=[q for q in qs.values() if q]
            for q in act:
                q[0][0]-=STEP/LINK/len(act)
                if q[0][0]<=1e-9:
                    heapq.heappush(pend,(now+LAT,q[0][1],q[0][2])); q.pop(0)
        now+=STEP
    return fwd,recv,acts,items,nitem,end,stall,arr

def encode():
    fwd, recv, acts, items, nitem, _, _, _ = plan()
    code = lambda me, g, p: g * NP + (0 if p == WHOLE else p) + 64 * sum(1 << f for f in fwd[me].get(g, ())) + 2048 * (p == WHOLE)
    npos = max(nitem) + len(PRE) + 1
    look = [[[0] * NDEV for _ in range(npos)] for _ in range(KS // 2)]
    for me in range(NDEV):
        for pos, ks in enumerate(acts[me]):
            assert len(ks) <= KS
            for k, (g, p) in enumerate(ks):
                look[k // 2][pos][me] += (code(me, g, p) + 1) << (13 * (k % 2))
    item = [[(items[me][w][0] * 32 + items[me][w][1]) if w < nitem[me] else 0 for me in range(NDEV)] for w in range(max(nitem))]
    firsts = [[code(me, own(me)[c], 0) for me in range(NDEV)] for c in (0, 1)]
    sent = []
    for f in range(5):
        lists = [sorted(g for g, fl in fwd[me].items() if f in fl) for me in range(NDEV)]
        for i in range(max(map(len, lists))):
            sent.append((f, [l[i] if i < len(l) else -1 for l in lists]))
    return look, item, firsts, sent


LOOK, ITEM, FIRST, SENT = encode()


def pick(me, row):
    common = max(set(row), key=lambda v: (row.count(v), v))
    out = jnp.int32(common)
    for i, v in enumerate(row):
        if v != common:
            out = jnp.where(me == i, jnp.int32(v), out)
    return out


def entry(values, at):
    if isinstance(at, int):
        return values[at]
    out = values[-1]
    for i, v in enumerate(values[:-1]):
        out = jnp.where(at == i, v, out)
    return out


def rope_tables():
    half = HD // 2
    freq = (np.float32(1.0) / np.power(np.float32(ROPE_BASE), np.arange(half, dtype=np.float32) * np.float32(2.0 / HD))).astype(np.float64)
    sign = np.concatenate([-np.ones(half), np.ones(half)])
    freq = np.concatenate([freq, freq])
    row = np.arange(CHUNK)[:, None] * freq
    base = (np.arange(NCH) * CHUNK)[:, None] * freq
    tabs = np.cos(row), np.sin(row) * sign, np.cos(base), np.sin(base) * sign
    return [t.astype(np.float32) for t in tabs]


def kernel(x_hbm, wq_hbm, wk_hbm, wv_hbm, cr_hbm, sr_hbm, cg_hbm, sg_hbm, o_ref,
           x, wq3, wq, wk, wv, cr, sr, cg, sg, cos, sin, kv, q, flat, s_scr, p_scr, mx_scr, al_scr, m_ref, l_ref, acc, tri,
           in_sem, send_sem, recv_sem):
    me = lax.axis_index('cp')
    core = lax.rem(me, 2)
    y = lax.rem(lax.div(me, 2), 2)

    loads = [(wk_hbm, wk), (wv_hbm, wv), (cr_hbm, cr), (sr_hbm, sr), (cg_hbm, cg), (sg_hbm, sg), (wq_hbm, wq3)]
    loads = [pltpu.make_async_copy(a, b, in_sem.at[i]) for i, (a, b) in enumerate(loads)]

    def load_x(c):
        rows = pl.ds(pl.multiple_of(c * CHUNK, CHUNK), CHUNK)
        return pltpu.make_async_copy(x_hbm.at[rows], x.at[rows], in_sem.at[7 + c])

    for cp in loads[:2] + [load_x(0)] + loads[2:6] + [load_x(1)] + loads[6:]:
        cp.start()

    sib = me + 1 - 2 * core
    mate = me + 2 - 4 * y
    bar = pltpu.get_barrier_semaphore()
    pl.semaphore_signal(bar, inc=1, device_id={'cp': sib}, device_id_type=pl.DeviceIdType.MESH)
    pl.semaphore_signal(bar, inc=1, device_id={'cp': mate}, device_id_type=pl.DeviceIdType.MESH)

    @pl.when(me + 4 < NDEV)
    def _():
        pl.semaphore_signal(bar, inc=1, device_id={'cp': me + 4}, device_id_type=pl.DeviceIdType.MESH)

    @pl.when(me >= 4)
    def _():
        pl.semaphore_signal(bar, inc=1, device_id={'cp': me - 4}, device_id_type=pl.DeviceIdType.MESH)

    looks = [[pick(me, row) for row in word] for word in LOOK]
    item = [pick(me, row) for row in ITEM]
    first = [pick(me, row) for row in FIRST]
    sent = [(f, pick(me, row)) for f, row in SENT]

    def copy_to(piece, f):
        to = (sib, me + 4, me - 4, me + 2, me - 2)[f]
        g, p = lax.div(piece, NP), lax.rem(piece, NP)
        part = kv.at[g, pl.ds(pl.multiple_of(p * CHUNK, CHUNK), CHUNK)]
        return pltpu.make_async_remote_copy(
            src_ref=part, dst_ref=part, send_sem=send_sem.at[f, g], recv_sem=recv_sem.at[piece],
            device_id={'cp': to}, device_id_type=pl.DeviceIdType.MESH)

    def send_on(code, pieces=1):
        piece, flags = lax.rem(code, 64), lax.div(code, 64)
        for f in range(5):
            @pl.when(lax.rem(lax.div(flags, 1 << f), 2) == 1)
            def _():
                for p in range(pieces):
                    copy_to(piece + p, f).start()

    def actions(pos):
        for word in looks:
            packed = entry(word, pos)

            @pl.when(packed > 0)
            def _():
                for k in range(2):
                    code = lax.rem(lax.div(packed, 1 << (13 * k)), 1 << 13) - 1

                    @pl.when((code >= 0) & (code < 2048))
                    def _():
                        copy_to(lax.rem(code, 64), 0).wait_recv()
                        send_on(code)

                    @pl.when(code >= 2048)
                    def _():
                        piece = lax.rem(code, 64)
                        for p in range(NP):
                            copy_to(piece + p, 0).wait_recv()

                        @pl.when(lax.rem(lax.div(code, 64), 2) == 1)
                        def _():
                            for p in range(NP):
                                copy_to(piece + p, 0).start()

    def own_chunk(c):
        return me + c * (NCH - 1 - 2 * me)

    def rope(v, c, rows):
        v = v.astype(jnp.bfloat16).astype(jnp.float32)
        return v * cos[c, rows] + pltpu.roll(v, HD // 2, 1) * sin[c, rows]

    for cp in loads[:6]:
        cp.wait()
    @pl.loop(0, 2)
    def _(c):
        g = own_chunk(c)
        cgr, sgr = cg[pl.ds(g, 1), :], sg[pl.ds(g, 1), :]
        cos[c] = cgr * cr[...] - sgr * sr[...]
        sin[c] = sgr * cr[...] + cgr * sr[...]
        load_x(c).wait()
        wkv = jnp.concatenate([wk[...], wv[...]], axis=1)
        both = jnp.dot(x[pl.ds(pl.multiple_of(c * CHUNK, CHUNK), CHUNK), :], wkv, preferred_element_type=jnp.float32)
        kv[g, pl.ds(0, CHUNK), :] = rope(both[:, :HD], c, slice(0, CHUNK)).astype(jnp.bfloat16)
        for b in range(0, CHUNK, HD):
            kv[g, pl.ds(CHUNK + b, HD), :] = both[b:b + HD, HD:].T.astype(jnp.bfloat16)

        @pl.when(c == 0)
        def _():
            pl.semaphore_wait(bar, 2 + jnp.where(me + 4 < NDEV, 1, 0) + jnp.where(me >= 4, 1, 0))

        send_on(jnp.where(c == 0, first[0], first[1]), NP)

    loads[6].wait()

    @pl.loop(0, DIM // TILE)
    def _(i):
        flat[...] = wq3[pl.ds(pl.multiple_of(i * HEADS * TILE, HEADS * TILE), HEADS * TILE), :].astype(jnp.float32)
        rows = pl.ds(pl.multiple_of(i * TILE, TILE), TILE)
        for h in range(HEADS):
            wq[rows, pl.ds(h * HD, HD)] = flat[pl.ds(h, TILE, stride=HEADS), :].astype(jnp.bfloat16)

    for c in range(2):
        if c == 1:
            actions(0)
        qs = jnp.dot(x[pl.ds(c * CHUNK, CHUNK), :], wq[...], preferred_element_type=jnp.float32)
        for h in range(HEADS):
            for r in range(2):
                rows = slice(r * TILE, (r + 1) * TILE)
                rot = rope(qs[rows, h * HD:(h + 1) * HD], c, rows)
                q[c * NT + h * 2 + r] = (rot * np.float32(HD ** -0.5)).astype(jnp.bfloat16)

    def scores(c, g, t, slot, k0=0, kn=CHUNK, bias=()):
        s = lax.dot_general(kv[g, pl.ds(k0, kn), :], q[c * NT + t], (((1,), (1,)), ((), ())), preferred_element_type=jnp.float32)
        parts = [s] if not bias else [s[i * TILE:(i + 1) * TILE] + b if b is not None else s[i * TILE:(i + 1) * TILE] for i, b in enumerate(bias)]
        tops = []
        for i, part in enumerate(parts):
            rows = part.shape[0]
            s_scr[slot, pl.ds(i * TILE, rows), :] = part
            tops.append(jnp.max(part.reshape(rows // 8, 8, TILE), axis=0))
        mx_scr[slot] = functools.reduce(jnp.maximum, tops)

    def softmax(c, t, slot, kn=CHUNK, first=False):
        n = c * NT + t
        mx = jnp.max(mx_scr[slot], axis=0, keepdims=True)
        if first:
            m_new = mx
        else:
            m_prev = m_ref[n]
            m_new = jnp.maximum(m_prev, mx)
            alpha = jnp.exp(m_prev - m_new)
            al_scr[slot] = alpha
        m_ref[n] = m_new
        p = jnp.exp(s_scr[slot, pl.ds(0, kn), :] - m_new)
        p_scr[slot, pl.ds(0, kn), :] = p.astype(jnp.bfloat16)
        part = jnp.sum(p.reshape(kn // 8, 8, TILE), axis=0)
        l_ref[n] = part if first else l_ref[n] * alpha + part

    def values(c, g, t, slot, k0=0, kn=CHUNK, first=False, last=False):
        vt = jnp.concatenate([kv[g, pl.ds(CHUNK + k0 + b, HD), :] for b in range(0, kn, HD)], axis=1)
        pv = jnp.dot(vt, p_scr[slot, pl.ds(0, kn), :], preferred_element_type=jnp.float32)
        n = c * NT + t
        total = pv if first else acc[n] * al_scr[slot] + pv
        if not last:
            acc[n] = total
            return
        h, r = t // 2, t % 2
        out = total / jnp.sum(l_ref[n], axis=0, keepdims=True)
        o_ref[pl.ds(c * CHUNK + r * TILE, TILE), pl.ds(h * HD, HD)] = out.T.astype(jnp.bfloat16)

    key_i = lax.broadcasted_iota(jnp.int32, (TILE, TILE), 0)
    row_i = lax.broadcasted_iota(jnp.int32, (TILE, TILE), 1)
    none = jnp.where(me < 8, TILE, 0)
    tri[0] = jnp.where(key_i <= row_i, 0.0, -jnp.inf)
    tri[1] = jnp.where(key_i > row_i, 0.0, -jnp.inf)
    tri[2] = jnp.where(key_i > row_i + none, 0.0, -jnp.inf)
    low_far = jnp.where(me < 8, jnp.float32(-jnp.inf), jnp.float32(0.0))

    def edge_blocks(far):
        def span(i):
            r, low = i % 2, i < NT
            if far:
                edge = tri[2] if low else tri[1]
                return (0, CHUNK, (edge, low_far if low else None)) if r == 0 else (TILE, TILE, (edge,))
            return (0, TILE, (tri[0],)) if r == 0 else (0, CHUNK, (None, tri[0]))

        chunk = [jnp.maximum(own_chunk(c) - 8, 0) if far else own_chunk(c) for c in range(2)]
        for i in range(2 * NT + AHEAD + 1):
            if i < 2 * NT:
                scores(i // NT, chunk[i // NT], i % NT, i % SLOTS, *span(i))
            j = i - AHEAD - 1
            if j >= 0:
                values(j // NT, chunk[j // NT], j % NT, j % SLOTS, *span(j)[:2], first=not far, last=far)
            j = i - AHEAD
            if 0 <= j < 2 * NT:
                softmax(j // NT, j % NT, j % SLOTS, span(j)[1], first=not far)

    actions(1)
    edge_blocks(False)

    n_full = jnp.minimum(me, 7) + 7
    actions(2)

    def c_and_g(code):
        return lax.div(code, 32), lax.rem(code, 32)

    c0, g0 = c_and_g(item[0])
    for t in range(AHEAD):
        scores(c0, g0, t, t)
    p_scr[SLOTS - 1] = jnp.zeros(p_scr.shape[1:], jnp.bfloat16)
    al_scr[SLOTS - 1] = jnp.ones(al_scr.shape[1:], jnp.float32)

    def full_block(w, carry):
        before, now = carry
        actions(w + len(PRE))
        after = jnp.where(w + 1 < n_full, entry(item, w + 1), now)
        c, g = c_and_g(now)
        cn, gn = c_and_g(after)
        cp, gp = c_and_g(before)
        for t in range(NT):
            a = t + AHEAD
            if a < NT:
                scores(c, g, a, a % SLOTS)
            else:
                scores(cn, gn, a - NT, a % SLOTS)
            if t == 0:
                values(cp, gp, NT - 1, SLOTS - 1)
            else:
                values(c, g, t - 1, (t - 1) % SLOTS)
            softmax(c, t, t % SLOTS)
        return now, after

    cl, gl = c_and_g(lax.fori_loop(0, n_full, full_block, (item[0], item[0]))[0])
    values(cl, gl, NT - 1, SLOTS - 1)
    actions(n_full + len(PRE))

    edge_blocks(True)

    for f, g in sent:
        @pl.when(g >= 0)
        def _():
            pltpu.make_async_remote_copy(
                src_ref=kv.at[g], dst_ref=kv.at[g], send_sem=send_sem.at[f, g], recv_sem=recv_sem.at[g * NP],
                device_id={'cp': sib}, device_id_type=pl.DeviceIdType.MESH).wait_send()


def attend(hidden, w_q, w_k, w_v):
    any_spec = pl.BlockSpec(memory_space=pl.ANY)
    f32, bf16 = jnp.float32, jnp.bfloat16
    return pl.pallas_call(
        kernel,
        out_shape=pltpu.VMEM((2 * CHUNK, HEADS * HD), bf16),
        in_specs=[any_spec] * 8,
        out_specs=pl.BlockSpec(memory_space=pltpu.VMEM),
        scratch_shapes=[
            pltpu.VMEM((2 * CHUNK, DIM), bf16),
            pltpu.VMEM((DIM * HEADS, HD), bf16),
            pltpu.VMEM((DIM, HEADS * HD), bf16),
            pltpu.VMEM((DIM, HD), bf16),
            pltpu.VMEM((DIM, HD), bf16),
            pltpu.VMEM((CHUNK, HD), f32),
            pltpu.VMEM((CHUNK, HD), f32),
            pltpu.VMEM((NCH, HD), f32),
            pltpu.VMEM((NCH, HD), f32),
            pltpu.VMEM((2, CHUNK, HD), f32),
            pltpu.VMEM((2, CHUNK, HD), f32),
            pltpu.VMEM((NCH, 2 * CHUNK, HD), bf16),
            pltpu.VMEM((2 * NT, TILE, HD), bf16),
            pltpu.VMEM((HEADS * TILE, HD), f32),
            pltpu.VMEM((SLOTS, CHUNK, TILE), f32),
            pltpu.VMEM((SLOTS, CHUNK, TILE), bf16),
            pltpu.VMEM((SLOTS, 8, TILE), f32),
            pltpu.VMEM((SLOTS, 1, TILE), f32),
            pltpu.VMEM((2 * NT, 1, TILE), f32),
            pltpu.VMEM((2 * NT, 8, TILE), f32),
            pltpu.VMEM((2 * NT, HD, TILE), f32),
            pltpu.VMEM((3, TILE, TILE), f32),
            pltpu.SemaphoreType.DMA((9,)),
            pltpu.SemaphoreType.DMA((5, NCH)),
            pltpu.SemaphoreType.DMA((NCH * NP,)),
        ],
        compiler_params=pltpu.CompilerParams(
            collective_id=0, has_side_effects=True, vmem_limit_bytes=56 << 20),
        cost_estimate=pl.CostEstimate(flops=15 * 10 ** 9, bytes_accessed=16 << 20, transcendentals=1 << 24),
    )(hidden, w_q.reshape(DIM * HEADS, HD), w_k.reshape(DIM, HD), w_v.reshape(DIM, HD), *rope_tables())


def project(heads, w_o):
    rows, cols = 256, 1024
    nr, nc = 2 * CHUNK // rows, DIM // cols

    def body(a, w, out, buf, sem):
        def store(i, j):
            part = pl.ds(i * rows, rows), pl.ds(j * cols, cols)
            return pltpu.make_async_copy(buf.at[part], out.at[part], sem.at[i, j])

        for i in range(nr):
            for j in range(nc):
                y = jnp.dot(a[pl.ds(i * rows, rows), :], w[:, pl.ds(j * cols, cols)], preferred_element_type=jnp.float32)
                buf[pl.ds(i * rows, rows), pl.ds(j * cols, cols)] = y.astype(jnp.bfloat16)
                store(i, j).start()
        for i in range(nr):
            for j in range(nc):
                store(i, j).wait()

    return pl.pallas_call(
        body,
        out_shape=jax.ShapeDtypeStruct((2 * CHUNK, DIM), jnp.bfloat16),
        in_specs=[pl.BlockSpec(memory_space=pltpu.VMEM)] * 2,
        out_specs=pl.BlockSpec(memory_space=pl.ANY),
        scratch_shapes=[pltpu.VMEM((2 * CHUNK, DIM), jnp.bfloat16), pltpu.SemaphoreType.DMA((nr, nc))],
        compiler_params=pltpu.CompilerParams(vmem_limit_bytes=32 << 20),
        cost_estimate=pl.CostEstimate(flops=4 * 2 ** 30, bytes_accessed=13 << 20, transcendentals=0),
    )(heads, pltpu.with_memory_space_constraint(w_o, pltpu.VMEM))


def solution(mesh):
    def device_step(hidden, w_q, w_k, w_v, w_o):
        heads = attend(hidden, w_q, w_k, w_v)
        return project(heads, w_o.reshape(HEADS * HD, DIM))

    from jax.sharding import PartitionSpec as P
    return jax.shard_map(device_step, mesh=mesh, in_specs=(P(('dp', 'cp'), None), P(), P(), P(), P()), out_specs=P(('dp', 'cp'), None), check_vma=False)
```

```python
import functools
import heapq

import jax
import jax.numpy as jnp
import numpy as np
from jax import lax
from jax.experimental import pallas as pl
from jax.experimental.pallas import tpu as pltpu

CHUNK, DIM, HD, HEADS = 512, 4096, 128, 4
TILE = 256
NT = HEADS * CHUNK // TILE
SLOTS, AHEAD = 4, 2
ROPE_BASE = 10000.0

NDEV, NCH = 16, 32
OFFS = (None, 4, -4, 2, -2)

def own(me): return (me, 31 - me)
def dst(me, f): return (me ^ 1) if f == 0 else me + OFFS[f]

def needs(me):
    s = set()
    for q in own(me):
        s |= {g for g in range(max(0, q - 8), q)}
    return s - set(own(me))

ACROSS = (0, 96)


def routes(across=None):
    low3, high3 = across or ACROSS
    fwd = [dict() for _ in range(NDEV)]
    def add(me, g, f):
        fwd[me].setdefault(g, []).append(f)
    for me in range(NDEV):
        y, core = (me // 2) % 2, me % 2
        L, H = own(me)
        if me + 4 < 16: add(me, L, 1)
        if y == 0: add(me, L, 3)
        if core == 0 or me >= 12: add(me, L, 0)
        if me >= 14: add(me, L, 4); add(me, L, 2)
        if me - 4 >= 0: add(me, H, 2)
        if y == 1: add(me, H, 4)
        if core == 1: add(me, H, 0)
        for d in (1, 2, 3, 4):
            g = me - 2 * d
            if g >= 0:
                by_y = (low3 >> (g // 2)) & 1
                ys = (g // 2) % 2
                if me + 4 < 16 and (d == 2 or (d == 1 and not by_y)): add(me, g, 1)
                if d == 2 and y == 1: add(me, g, 4)
                if by_y and d == 2 and ys == 0: add(me, g, 3)
                if by_y and d == 4 and ys == 1: add(me, g, 4)
                if by_y and ys == 1 and d == 1 and me + 4 >= 12 and me + 6 > 15 and me + 4 < 16: add(me, g, 1)
                if d == 1 and me >= 14: add(me, g, 2)
                if d < 4 or core == 1: add(me, g, 0)
            if me + 2 * d < 16:
                s = me + 2 * d
                h = 31 - s
                by_y = (high3 >> (s // 2)) & 1
                ys = (s // 2) % 2
                if me - 4 >= 0 and (d == 2 or (d == 1 and not by_y)): add(me, h, 2)
                if d == 2 and y == 0: add(me, h, 3)
                if by_y and d == 2 and ys == 1: add(me, h, 4)
                if by_y and d == 4 and ys == 0: add(me, h, 3)
                if by_y and ys == 0 and d == 1 and me - 6 < 0 and me - 4 >= 0: add(me, h, 2)
                if d < 4 or core == 0: add(me, h, 0)
        if me in (12, 13): add(me, me + 2, 2); add(me, me + 2, 0)
        if me in (10, 11): add(me, me + 2, 0); add(me, me + 4, 0)
        if me in (8, 9): add(me, me + 6, 0)
    return fwd


def check(fwd):
    recv = [dict() for _ in range(NDEV)]
    for me in range(NDEV):
        for g, fl in fwd[me].items():
            for f in fl:
                d = dst(me, f)
                assert 0 <= d < 16 and d != me, (me, g, f)
                assert g not in recv[d], (me, g, f, d, recv[d].get(g))
                assert g not in own(d)
                recv[d][g] = me
    for me in range(NDEV):
        for g in fwd[me]: assert g in own(me) or g in recv[me], (me, g)
        assert needs(me) <= set(recv[me]), (me, needs(me) - set(recv[me]))
    return recv


NP, KS = 2, 2
WHOLE = -1
PRE = (9.3, 11.9)
KVT, EDGE, DT, ACT_T, LINK, LAT, D2D, MARGIN, STEP = (4.3, 5.8), 2.1, 1.22, 0.05, 2.82, 1.9, 1.5, 0.3, 0.03


def plan():
    fwd = routes()
    recv = check(fwd)
    npre=len(PRE)
    dep={}
    def depth(me,g):
        k=(me,g)
        if k not in dep: dep[k]=max([0]+[(0.1 if f==0 else 1)+depth(dst(me,f),g) for f in fwd[me].get(g,())])
        return dep[k]
    need=[set() for _ in range(NDEV)]
    todo=[]
    for me in range(NDEV):
        todo.append([(c,g) for c,q in enumerate(own(me)) for g in range(max(0,q-7),q)])
    nitem=[len(t) for t in todo]
    acts=[[] for _ in range(NDEV)]; items=[[] for _ in range(NDEV)]
    held=[{(g,p) for g in own(m) for p in range(NP)} for m in range(NDEV)]
    arr=[dict() for _ in range(NDEV)]
    queue={}; pend=[]
    def send(me,g,p,now):
        for f in fwd[me].get(g,()):
            d=dst(me,f)
            if f==0: heapq.heappush(pend,(now+D2D,d,(g,p)))
            else: queue.setdefault((me//2,f),({0:[],1:[]}))[me%2].append([1.0/NP,d,(g,p)])
    def spread(ks): return {(g,r) for g,q in ks for r in range(NP) if q==WHOLE or q==r}
    started=[[False,False] for _ in range(NDEV)]
    clock=[PRE[0]]*NDEV; pos=[0]*NDEV; end=[None]*NDEV; stall=[0.0]*NDEV
    npiece=[len(recv[m])*NP for m in range(NDEV)]
    now=0.0
    while any(e is None for e in end):
        if now>90: return None
        while pend and pend[0][0]<=now:
            tt,d,k=heapq.heappop(pend); arr[d][k]=tt
        for me in range(NDEV):
            for c in (0,1):
                if not started[me][c] and now>=KVT[c]:
                    started[me][c]=True
                    for p in range(NP): send(me,own(me)[c],p,now)
            if end[me] is not None or now<clock[me]: continue
            p=pos[me]; h=held[me]
            last=p==npre+nitem[me]
            def units(when):
                out=[]
                for g in {k[0] for k in arr[me] if k not in h}:
                    if any(f for f in fwd[me].get(g,())):
                        out+=[(arr[me][(g,q)],g,q) for q in range(NP) if (g,q) in arr[me] and (g,q) not in h and arr[me][(g,q)]<=when]
                    elif all((g,q) in arr[me] for q in range(NP)):
                        t=max(arr[me][(g,q)] for q in range(NP))
                        if t<=when: out.append((t,g,WHOLE))
                return out
            take=[(g,q) for t,g,q in sorted(units(now-MARGIN),key=lambda u:(-depth(me,u[1]),u[0],u[1],u[2]))[:KS]]
            if last:
                if len(h)-2*NP+len([k for k in arr[me] if k not in h])<npiece[me]: stall[me]+=STEP; continue
                take=[(g,q) for t,g,q in sorted(units(now))]
                if len(take)>KS: return None
            elif p>=npre-1 and p-npre+1<nitem[me]:
                def ok_items(t):
                    hh=h|spread(t)
                    return [it for it in todo[me] if all((it[1],q) in hh for q in range(NP))]
                ok=ok_items(take)
                if not ok:
                    full=[it for it in todo[me] if all((it[1],q) in h or (it[1],q) in arr[me] for q in range(NP))]
                    if not full: stall[me]+=STEP; continue
                    g=min(full,key=lambda it:max(arr[me].get((it[1],q),0) for q in range(NP)))[1]
                    must=[(g2,q) for t,g2,q in units(now) if g2==g]
                    take=(must+[k for k in take if k not in must])[:KS]
                    ok=ok_items(take)
                rem=[sum(1 for it in todo[me] if it[0]==c) for c in (0,1)]
                lead=0 if rem[0]>=rem[1] else 1
                it=sorted(ok,key=lambda it:it[0]!=lead)[0]
                todo[me].remove(it); items[me].append(it)
            acts[me].append(take)
            h|=spread(take)
            for g,q in sorted(spread(take)): send(me,g,q,now)
            if last: end[me]=now; continue
            pos[me]+=1
            if p+1<npre: clock[me]=max(now,PRE[p+1])
            else: clock[me]=now+ACT_T*len(take)+(EDGE if p+1==npre else DT)
        for k,qs in queue.items():
            act=[q for q in qs.values() if q]
            for q in act:
                q[0][0]-=STEP/LINK/len(act)
                if q[0][0]<=1e-9:
                    heapq.heappush(pend,(now+LAT,q[0][1],q[0][2])); q.pop(0)
        now+=STEP
    return fwd,recv,acts,items,nitem,end,stall,arr

def encode():
    fwd, recv, acts, items, nitem, _, _, _ = plan()
    code = lambda me, g, p: g * NP + (0 if p == WHOLE else p) + 64 * sum(1 << f for f in fwd[me].get(g, ())) + 2048 * (p == WHOLE)
    npos = max(nitem) + len(PRE) + 1
    look = [[[0] * NDEV for _ in range(npos)] for _ in range(KS // 2)]
    for me in range(NDEV):
        for pos, ks in enumerate(acts[me]):
            assert len(ks) <= KS
            for k, (g, p) in enumerate(ks):
                look[k // 2][pos][me] += (code(me, g, p) + 1) << (13 * (k % 2))
    item = [[(items[me][w][0] * 32 + items[me][w][1]) if w < nitem[me] else 0 for me in range(NDEV)] for w in range(max(nitem))]
    firsts = [[code(me, own(me)[c], 0) for me in range(NDEV)] for c in (0, 1)]
    sent = []
    for f in range(5):
        lists = [sorted(g for g, fl in fwd[me].items() if f in fl) for me in range(NDEV)]
        for i in range(max(map(len, lists))):
            sent.append((f, [l[i] if i < len(l) else -1 for l in lists]))
    return look, item, firsts, sent


LOOK, ITEM, FIRST, SENT = encode()


def pick(me, row):
    common = max(set(row), key=lambda v: (row.count(v), v))
    out = jnp.int32(common)
    for i, v in enumerate(row):
        if v != common:
            out = jnp.where(me == i, jnp.int32(v), out)
    return out


def entry(values, at):
    if isinstance(at, int):
        return values[at]
    out = values[-1]
    for i, v in enumerate(values[:-1]):
        out = jnp.where(at == i, v, out)
    return out


def rope_tables():
    half = HD // 2
    freq = (np.float32(1.0) / np.power(np.float32(ROPE_BASE), np.arange(half, dtype=np.float32) * np.float32(2.0 / HD))).astype(np.float64)
    sign = np.concatenate([-np.ones(half), np.ones(half)])
    freq = np.concatenate([freq, freq])
    row = np.arange(CHUNK)[:, None] * freq
    base = (np.arange(NCH) * CHUNK)[:, None] * freq
    tabs = np.cos(row), np.sin(row) * sign, np.cos(base), np.sin(base) * sign
    return [t.astype(np.float32) for t in tabs]


def kernel(x_hbm, wq_hbm, wk_hbm, wv_hbm, cr_hbm, sr_hbm, cg_hbm, sg_hbm, o_ref,
           x, wq3, wq, wk, wv, cr, sr, cg, sg, cos, sin, kv, q, flat, s_scr, p_scr, mx_scr, al_scr, m_ref, l_ref, acc, tri,
           in_sem, send_sem, recv_sem):
    me = lax.axis_index('cp')
    core = lax.rem(me, 2)
    y = lax.rem(lax.div(me, 2), 2)

    loads = [(wk_hbm, wk), (wv_hbm, wv), (cr_hbm, cr), (sr_hbm, sr), (cg_hbm, cg), (sg_hbm, sg), (wq_hbm, wq3)]
    loads = [pltpu.make_async_copy(a, b, in_sem.at[i]) for i, (a, b) in enumerate(loads)]

    def load_x(c):
        rows = pl.ds(pl.multiple_of(c * CHUNK, CHUNK), CHUNK)
        return pltpu.make_async_copy(x_hbm.at[rows], x.at[rows], in_sem.at[7 + c])

    for cp in loads[:2] + [load_x(0)] + loads[2:6] + [load_x(1)] + loads[6:]:
        cp.start()

    sib = me + 1 - 2 * core
    mate = me + 2 - 4 * y
    bar = pltpu.get_barrier_semaphore()
    pl.semaphore_signal(bar, inc=1, device_id={'cp': sib}, device_id_type=pl.DeviceIdType.MESH)
    pl.semaphore_signal(bar, inc=1, device_id={'cp': mate}, device_id_type=pl.DeviceIdType.MESH)

    @pl.when(me + 4 < NDEV)
    def _():
        pl.semaphore_signal(bar, inc=1, device_id={'cp': me + 4}, device_id_type=pl.DeviceIdType.MESH)

    @pl.when(me >= 4)
    def _():
        pl.semaphore_signal(bar, inc=1, device_id={'cp': me - 4}, device_id_type=pl.DeviceIdType.MESH)

    looks = [[pick(me, row) for row in word] for word in LOOK]
    item = [pick(me, row) for row in ITEM]
    first = [pick(me, row) for row in FIRST]
    sent = [(f, pick(me, row)) for f, row in SENT]

    def copy_to(piece, f):
        to = (sib, me + 4, me - 4, me + 2, me - 2)[f]
        g, p = lax.div(piece, NP), lax.rem(piece, NP)
        part = kv.at[g, pl.ds(pl.multiple_of(p * CHUNK, CHUNK), CHUNK)]
        return pltpu.make_async_remote_copy(
            src_ref=part, dst_ref=part, send_sem=send_sem.at[f, g], recv_sem=recv_sem.at[piece],
            device_id={'cp': to}, device_id_type=pl.DeviceIdType.MESH)

    def send_on(code, pieces=1):
        piece, flags = lax.rem(code, 64), lax.div(code, 64)
        for f in range(5):
            @pl.when(lax.rem(lax.div(flags, 1 << f), 2) == 1)
            def _():
                for p in range(pieces):
                    copy_to(piece + p, f).start()

    def actions(pos):
        for word in looks:
            packed = entry(word, pos)

            @pl.when(packed > 0)
            def _():
                for k in range(2):
                    code = lax.rem(lax.div(packed, 1 << (13 * k)), 1 << 13) - 1

                    @pl.when((code >= 0) & (code < 2048))
                    def _():
                        copy_to(lax.rem(code, 64), 0).wait_recv()
                        send_on(code)

                    @pl.when(code >= 2048)
                    def _():
                        piece = lax.rem(code, 64)
                        for p in range(NP):
                            copy_to(piece + p, 0).wait_recv()

                        @pl.when(lax.rem(lax.div(code, 64), 2) == 1)
                        def _():
                            for p in range(NP):
                                copy_to(piece + p, 0).start()

    def own_chunk(c):
        return me + c * (NCH - 1 - 2 * me)

    def rope(v, c, rows):
        v = v.astype(jnp.bfloat16).astype(jnp.float32)
        return v * cos[c, rows] + pltpu.roll(v, HD // 2, 1) * sin[c, rows]

    for cp in loads[:6]:
        cp.wait()
    @pl.loop(0, 2)
    def _(c):
        g = own_chunk(c)
        cgr, sgr = cg[pl.ds(g, 1), :], sg[pl.ds(g, 1), :]
        cos[c] = cgr * cr[...] - sgr * sr[...]
        sin[c] = sgr * cr[...] + cgr * sr[...]
        load_x(c).wait()
        wkv = jnp.concatenate([wk[...], wv[...]], axis=1)
        both = jnp.dot(x[pl.ds(pl.multiple_of(c * CHUNK, CHUNK), CHUNK), :], wkv, preferred_element_type=jnp.float32)
        kv[g, pl.ds(0, CHUNK), :] = rope(both[:, :HD], c, slice(0, CHUNK)).astype(jnp.bfloat16)
        for b in range(0, CHUNK, HD):
            kv[g, pl.ds(CHUNK + b, HD), :] = both[b:b + HD, HD:].T.astype(jnp.bfloat16)

        @pl.when(c == 0)
        def _():
            pl.semaphore_wait(bar, 2 + jnp.where(me + 4 < NDEV, 1, 0) + jnp.where(me >= 4, 1, 0))

        send_on(jnp.where(c == 0, first[0], first[1]), NP)

    loads[6].wait()

    @pl.loop(0, DIM // TILE)
    def _(i):
        flat[...] = wq3[pl.ds(pl.multiple_of(i * HEADS * TILE, HEADS * TILE), HEADS * TILE), :].astype(jnp.float32)
        rows = pl.ds(pl.multiple_of(i * TILE, TILE), TILE)
        for h in range(HEADS):
            wq[rows, pl.ds(h * HD, HD)] = flat[pl.ds(h, TILE, stride=HEADS), :].astype(jnp.bfloat16)

    for c in range(2):
        if c == 1:
            actions(0)
        qs = jnp.dot(x[pl.ds(c * CHUNK, CHUNK), :], wq[...], preferred_element_type=jnp.float32)
        for h in range(HEADS):
            for r in range(2):
                rows = slice(r * TILE, (r + 1) * TILE)
                rot = rope(qs[rows, h * HD:(h + 1) * HD], c, rows)
                q[c * NT + h * 2 + r] = (rot * np.float32(HD ** -0.5)).astype(jnp.bfloat16)

    def scores(c, g, t, slot, k0=0, kn=CHUNK, bias=()):
        s = lax.dot_general(kv[g, pl.ds(k0, kn), :], q[c * NT + t], (((1,), (1,)), ((), ())), preferred_element_type=jnp.float32)
        parts = [s] if not bias else [s[i * TILE:(i + 1) * TILE] + b if b is not None else s[i * TILE:(i + 1) * TILE] for i, b in enumerate(bias)]
        tops = []
        for i, part in enumerate(parts):
            rows = part.shape[0]
            s_scr[slot, pl.ds(i * TILE, rows), :] = part
            tops.append(jnp.max(part.reshape(rows // 8, 8, TILE), axis=0))
        mx_scr[slot] = functools.reduce(jnp.maximum, tops)

    def softmax(c, t, slot, kn=CHUNK, first=False):
        n = c * NT + t
        mx = jnp.max(mx_scr[slot], axis=0, keepdims=True)
        if first:
            m_new = mx
        else:
            m_prev = m_ref[n]
            m_new = jnp.maximum(m_prev, mx)
            alpha = jnp.exp(m_prev - m_new)
            al_scr[slot] = alpha
        m_ref[n] = m_new
        p = jnp.exp(s_scr[slot, pl.ds(0, kn), :] - m_new)
        p_scr[slot, pl.ds(0, kn), :] = p.astype(jnp.bfloat16)
        part = jnp.sum(p.reshape(kn // 8, 8, TILE), axis=0)
        l_ref[n] = part if first else l_ref[n] * alpha + part

    def values(c, g, t, slot, k0=0, kn=CHUNK, first=False, last=False):
        vt = jnp.concatenate([kv[g, pl.ds(CHUNK + k0 + b, HD), :] for b in range(0, kn, HD)], axis=1)
        pv = jnp.dot(vt, p_scr[slot, pl.ds(0, kn), :], preferred_element_type=jnp.float32)
        n = c * NT + t
        total = pv if first else acc[n] * al_scr[slot] + pv
        if not last:
            acc[n] = total
            return
        h, r = t // 2, t % 2
        out = total / jnp.sum(l_ref[n], axis=0, keepdims=True)
        o_ref[pl.ds(c * CHUNK + r * TILE, TILE), pl.ds(h * HD, HD)] = out.T.astype(jnp.bfloat16)

    key_i = lax.broadcasted_iota(jnp.int32, (TILE, TILE), 0)
    row_i = lax.broadcasted_iota(jnp.int32, (TILE, TILE), 1)
    none = jnp.where(me < 8, TILE, 0)
    tri[0] = jnp.where(key_i <= row_i, 0.0, -jnp.inf)
    tri[1] = jnp.where(key_i > row_i, 0.0, -jnp.inf)
    tri[2] = jnp.where(key_i > row_i + none, 0.0, -jnp.inf)
    low_far = jnp.where(me < 8, jnp.float32(-jnp.inf), jnp.float32(0.0))

    def edge_blocks(far, then=None):
        def span(i):
            r, low = i % 2, i < NT
            if far:
                edge = tri[2] if low else tri[1]
                return (0, CHUNK, (edge, low_far if low else None)) if r == 0 else (TILE, TILE, (edge,))
            return (0, TILE, (tri[0],)) if r == 0 else (0, CHUNK, (None, tri[0]))

        chunk = [jnp.maximum(own_chunk(c) - 8, 0) if far else own_chunk(c) for c in range(2)]
        for i in range(2 * NT + AHEAD + 1):
            if then is not None and 2 * NT <= i < 2 * NT + AHEAD:
                scores(*then, i - 2 * NT, i % SLOTS)
            if i < 2 * NT:
                scores(i // NT, chunk[i // NT], i % NT, i % SLOTS, *span(i))
            j = i - AHEAD - 1
            if j >= 0:
                values(j // NT, chunk[j // NT], j % NT, j % SLOTS, *span(j)[:2], first=not far, last=far)
            j = i - AHEAD
            if 0 <= j < 2 * NT:
                softmax(j // NT, j % NT, j % SLOTS, span(j)[1], first=not far)

    def c_and_g(code):
        return lax.div(code, 32), lax.rem(code, 32)

    n_full = jnp.minimum(me, 7) + 7
    actions(1)
    edge_blocks(False, then=c_and_g(item[0]))
    p_scr[SLOTS - 1] = jnp.zeros(p_scr.shape[1:], jnp.bfloat16)
    al_scr[SLOTS - 1] = jnp.ones(al_scr.shape[1:], jnp.float32)

    def full_block(w, carry):
        before, now = carry
        actions(w + len(PRE))
        after = jnp.where(w + 1 < n_full, entry(item, w + 1), now)
        c, g = c_and_g(now)
        cn, gn = c_and_g(after)
        cp, gp = c_and_g(before)
        for t in range(NT):
            a = t + AHEAD
            if a < NT:
                scores(c, g, a, a % SLOTS)
            else:
                scores(cn, gn, a - NT, a % SLOTS)
            if t == 0:
                values(cp, gp, NT - 1, SLOTS - 1)
            else:
                values(c, g, t - 1, (t - 1) % SLOTS)
            softmax(c, t, t % SLOTS)
        return now, after

    cl, gl = c_and_g(lax.fori_loop(0, n_full, full_block, (item[0], item[0]))[0])
    actions(n_full + len(PRE))
    values(cl, gl, NT - 1, SLOTS - 1)
    edge_blocks(True)

    for f, g in sent:
        @pl.when(g >= 0)
        def _():
            pltpu.make_async_remote_copy(
                src_ref=kv.at[g], dst_ref=kv.at[g], send_sem=send_sem.at[f, g], recv_sem=recv_sem.at[g * NP],
                device_id={'cp': sib}, device_id_type=pl.DeviceIdType.MESH).wait_send()


def attend(hidden, w_q, w_k, w_v):
    any_spec = pl.BlockSpec(memory_space=pl.ANY)
    f32, bf16 = jnp.float32, jnp.bfloat16
    return pl.pallas_call(
        kernel,
        out_shape=pltpu.VMEM((2 * CHUNK, HEADS * HD), bf16),
        in_specs=[any_spec] * 8,
        out_specs=pl.BlockSpec(memory_space=pltpu.VMEM),
        scratch_shapes=[
            pltpu.VMEM((2 * CHUNK, DIM), bf16),
            pltpu.VMEM((DIM * HEADS, HD), bf16),
            pltpu.VMEM((DIM, HEADS * HD), bf16),
            pltpu.VMEM((DIM, HD), bf16),
            pltpu.VMEM((DIM, HD), bf16),
            pltpu.VMEM((CHUNK, HD), f32),
            pltpu.VMEM((CHUNK, HD), f32),
            pltpu.VMEM((NCH, HD), f32),
            pltpu.VMEM((NCH, HD), f32),
            pltpu.VMEM((2, CHUNK, HD), f32),
            pltpu.VMEM((2, CHUNK, HD), f32),
            pltpu.VMEM((NCH, 2 * CHUNK, HD), bf16),
            pltpu.VMEM((2 * NT, TILE, HD), bf16),
            pltpu.VMEM((HEADS * TILE, HD), f32),
            pltpu.VMEM((SLOTS, CHUNK, TILE), f32),
            pltpu.VMEM((SLOTS, CHUNK, TILE), bf16),
            pltpu.VMEM((SLOTS, 8, TILE), f32),
            pltpu.VMEM((SLOTS, 1, TILE), f32),
            pltpu.VMEM((2 * NT, 1, TILE), f32),
            pltpu.VMEM((2 * NT, 8, TILE), f32),
            pltpu.VMEM((2 * NT, HD, TILE), f32),
            pltpu.VMEM((3, TILE, TILE), f32),
            pltpu.SemaphoreType.DMA((9,)),
            pltpu.SemaphoreType.DMA((5, NCH)),
            pltpu.SemaphoreType.DMA((NCH * NP,)),
        ],
        compiler_params=pltpu.CompilerParams(
            collective_id=0, has_side_effects=True, vmem_limit_bytes=56 << 20),
        cost_estimate=pl.CostEstimate(flops=15 * 10 ** 9, bytes_accessed=16 << 20, transcendentals=1 << 24),
    )(hidden, w_q.reshape(DIM * HEADS, HD), w_k.reshape(DIM, HD), w_v.reshape(DIM, HD), *rope_tables())


def project(heads, w_o):
    rows, cols = 256, 1024
    nr, nc = 2 * CHUNK // rows, DIM // cols

    def body(a, w, out, buf, sem):
        def store(i, j):
            part = pl.ds(i * rows, rows), pl.ds(j * cols, cols)
            return pltpu.make_async_copy(buf.at[part], out.at[part], sem.at[i, j])

        for i in range(nr):
            for j in range(nc):
                y = jnp.dot(a[pl.ds(i * rows, rows), :], w[:, pl.ds(j * cols, cols)], preferred_element_type=jnp.float32)
                buf[pl.ds(i * rows, rows), pl.ds(j * cols, cols)] = y.astype(jnp.bfloat16)
                store(i, j).start()
        for i in range(nr):
            for j in range(nc):
                store(i, j).wait()

    return pl.pallas_call(
        body,
        out_shape=jax.ShapeDtypeStruct((2 * CHUNK, DIM), jnp.bfloat16),
        in_specs=[pl.BlockSpec(memory_space=pltpu.VMEM)] * 2,
        out_specs=pl.BlockSpec(memory_space=pl.ANY),
        scratch_shapes=[pltpu.VMEM((2 * CHUNK, DIM), jnp.bfloat16), pltpu.SemaphoreType.DMA((nr, nc))],
        compiler_params=pltpu.CompilerParams(vmem_limit_bytes=32 << 20),
        cost_estimate=pl.CostEstimate(flops=4 * 2 ** 30, bytes_accessed=13 << 20, transcendentals=0),
    )(heads, pltpu.with_memory_space_constraint(w_o, pltpu.VMEM))


def solution(mesh):
    def device_step(hidden, w_q, w_k, w_v, w_o):
        heads = attend(hidden, w_q, w_k, w_v)
        return project(heads, w_o.reshape(HEADS * HD, DIM))

    from jax.sharding import PartitionSpec as P
    return jax.shard_map(device_step, mesh=mesh, in_specs=(P(('dp', 'cp'), None), P(), P(), P(), P()), out_specs=P(('dp', 'cp'), None), check_vma=False)
```

```python
import functools
import heapq

import jax
import jax.numpy as jnp
import numpy as np
from jax import lax
from jax.experimental import pallas as pl
from jax.experimental.pallas import tpu as pltpu

CHUNK, DIM, HD, HEADS = 512, 4096, 128, 4
TILE = 256
NT = HEADS * CHUNK // TILE
SLOTS, AHEAD = 4, 2
ROPE_BASE = 10000.0

NDEV, NCH = 16, 32
OFFS = (None, 4, -4, 2, -2)

def own(me): return (me, 31 - me)
def dst(me, f): return (me ^ 1) if f == 0 else me + OFFS[f]

def needs(me):
    s = set()
    for q in own(me):
        s |= {g for g in range(max(0, q - 8), q)}
    return s - set(own(me))

ACROSS = (0, 96)


def routes(across=None):
    low3, high3 = across or ACROSS
    fwd = [dict() for _ in range(NDEV)]
    def add(me, g, f):
        fwd[me].setdefault(g, []).append(f)
    for me in range(NDEV):
        y, core = (me // 2) % 2, me % 2
        L, H = own(me)
        if me + 4 < 16: add(me, L, 1)
        if y == 0: add(me, L, 3)
        if core == 0 or me >= 12: add(me, L, 0)
        if me >= 14: add(me, L, 4); add(me, L, 2)
        if me - 4 >= 0: add(me, H, 2)
        if y == 1: add(me, H, 4)
        if core == 1: add(me, H, 0)
        for d in (1, 2, 3, 4):
            g = me - 2 * d
            if g >= 0:
                by_y = (low3 >> (g // 2)) & 1
                ys = (g // 2) % 2
                if me + 4 < 16 and (d == 2 or (d == 1 and not by_y)): add(me, g, 1)
                if d == 2 and y == 1: add(me, g, 4)
                if by_y and d == 2 and ys == 0: add(me, g, 3)
                if by_y and d == 4 and ys == 1: add(me, g, 4)
                if by_y and ys == 1 and d == 1 and me + 4 >= 12 and me + 6 > 15 and me + 4 < 16: add(me, g, 1)
                if d == 1 and me >= 14: add(me, g, 2)
                if d < 4 or core == 1: add(me, g, 0)
            if me + 2 * d < 16:
                s = me + 2 * d
                h = 31 - s
                by_y = (high3 >> (s // 2)) & 1
                ys = (s // 2) % 2
                if me - 4 >= 0 and (d == 2 or (d == 1 and not by_y)): add(me, h, 2)
                if d == 2 and y == 0: add(me, h, 3)
                if by_y and d == 2 and ys == 1: add(me, h, 4)
                if by_y and d == 4 and ys == 0: add(me, h, 3)
                if by_y and ys == 0 and d == 1 and me - 6 < 0 and me - 4 >= 0: add(me, h, 2)
                if d < 4 or core == 0: add(me, h, 0)
        if me in (12, 13): add(me, me + 2, 2); add(me, me + 2, 0)
        if me in (10, 11): add(me, me + 2, 0); add(me, me + 4, 0)
        if me in (8, 9): add(me, me + 6, 0)
    return fwd


def check(fwd):
    recv = [dict() for _ in range(NDEV)]
    for me in range(NDEV):
        for g, fl in fwd[me].items():
            for f in fl:
                d = dst(me, f)
                assert 0 <= d < 16 and d != me, (me, g, f)
                assert g not in recv[d], (me, g, f, d, recv[d].get(g))
                assert g not in own(d)
                recv[d][g] = me
    for me in range(NDEV):
        for g in fwd[me]: assert g in own(me) or g in recv[me], (me, g)
        assert needs(me) <= set(recv[me]), (me, needs(me) - set(recv[me]))
    return recv


NP, KS = 2, 2
WHOLE = -1
PRE = (9.8, 12.6)
KVT, EDGE, DT, ACT_T, LINK, LAT, D2D, MARGIN, STEP = (4.4, 6.0), 2.2, 1.30, 0.05, 2.82, 1.9, 1.5, 0.8, 0.03


def plan():
    fwd = routes()
    recv = check(fwd)
    npre=len(PRE)
    dep={}
    def depth(me,g):
        k=(me,g)
        if k not in dep: dep[k]=max([0]+[(0.1 if f==0 else 1)+depth(dst(me,f),g) for f in fwd[me].get(g,())])
        return dep[k]
    need=[set() for _ in range(NDEV)]
    todo=[]
    for me in range(NDEV):
        todo.append([(c,g) for c,q in enumerate(own(me)) for g in range(max(0,q-7),q)])
    nitem=[len(t) for t in todo]
    acts=[[] for _ in range(NDEV)]; items=[[] for _ in range(NDEV)]
    held=[{(g,p) for g in own(m) for p in range(NP)} for m in range(NDEV)]
    arr=[dict() for _ in range(NDEV)]
    queue={}; pend=[]
    def send(me,g,p,now):
        for f in fwd[me].get(g,()):
            d=dst(me,f)
            if f==0: heapq.heappush(pend,(now+D2D,d,(g,p)))
            else: queue.setdefault((me//2,f),({0:[],1:[]}))[me%2].append([1.0/NP,d,(g,p)])
    def spread(ks): return {(g,r) for g,q in ks for r in range(NP) if q==WHOLE or q==r}
    started=[[False,False] for _ in range(NDEV)]
    clock=[PRE[0]]*NDEV; pos=[0]*NDEV; end=[None]*NDEV; stall=[0.0]*NDEV
    npiece=[len(recv[m])*NP for m in range(NDEV)]
    now=0.0
    while any(e is None for e in end):
        if now>90: return None
        while pend and pend[0][0]<=now:
            tt,d,k=heapq.heappop(pend); arr[d][k]=tt
        for me in range(NDEV):
            for c in (0,1):
                if not started[me][c] and now>=KVT[c]:
                    started[me][c]=True
                    for p in range(NP): send(me,own(me)[c],p,now)
            if end[me] is not None or now<clock[me]: continue
            p=pos[me]; h=held[me]
            last=p==npre+nitem[me]
            def units(when):
                out=[]
                for g in {k[0] for k in arr[me] if k not in h}:
                    if any(f for f in fwd[me].get(g,())):
                        out+=[(arr[me][(g,q)],g,q) for q in range(NP) if (g,q) in arr[me] and (g,q) not in h and arr[me][(g,q)]<=when]
                    elif all((g,q) in arr[me] for q in range(NP)):
                        t=max(arr[me][(g,q)] for q in range(NP))
                        if t<=when: out.append((t,g,WHOLE))
                return out
            take=[(g,q) for t,g,q in sorted(units(now-MARGIN),key=lambda u:(-depth(me,u[1]),u[0],u[1],u[2]))[:KS]]
            if last:
                if len(h)-2*NP+len([k for k in arr[me] if k not in h])<npiece[me]: stall[me]+=STEP; continue
                take=[(g,q) for t,g,q in sorted(units(now))]
                if len(take)>KS: return None
            elif p>=npre-1 and p-npre+1<nitem[me]:
                def ok_items(t):
                    hh=h|spread(t)
                    return [it for it in todo[me] if all((it[1],q) in hh for q in range(NP))]
                ok=ok_items(take)
                if not ok:
                    full=[it for it in todo[me] if all((it[1],q) in h or (it[1],q) in arr[me] for q in range(NP))]
                    if not full: stall[me]+=STEP; continue
                    g=min(full,key=lambda it:max(arr[me].get((it[1],q),0) for q in range(NP)))[1]
                    must=[(g2,q) for t,g2,q in units(now) if g2==g]
                    take=(must+[k for k in take if k not in must])[:KS]
                    ok=ok_items(take)
                rem=[sum(1 for it in todo[me] if it[0]==c) for c in (0,1)]
                lead=0 if rem[0]>=rem[1] else 1
                it=sorted(ok,key=lambda it:it[0]!=lead)[0]
                todo[me].remove(it); items[me].append(it)
            acts[me].append(take)
            h|=spread(take)
            for g,q in sorted(spread(take)): send(me,g,q,now)
            if last: end[me]=now; continue
            pos[me]+=1
            if p+1<npre: clock[me]=max(now,PRE[p+1])
            else: clock[me]=now+ACT_T*len(take)+(EDGE if p+1==npre else DT)
        for k,qs in queue.items():
            act=[q for q in qs.values() if q]
            for q in act:
                q[0][0]-=STEP/LINK/len(act)
                if q[0][0]<=1e-9:
                    heapq.heappush(pend,(now+LAT,q[0][1],q[0][2])); q.pop(0)
        now+=STEP
    return fwd,recv,acts,items,nitem,end,stall,arr

def encode():
    fwd, recv, acts, items, nitem, _, _, _ = plan()
    code = lambda me, g, p: g * NP + (0 if p == WHOLE else p) + 64 * sum(1 << f for f in fwd[me].get(g, ())) + 2048 * (p == WHOLE)
    npos = max(nitem) + len(PRE) + 1
    look = [[[0] * NDEV for _ in range(npos)] for _ in range(KS // 2)]
    for me in range(NDEV):
        for pos, ks in enumerate(acts[me]):
            assert len(ks) <= KS
            for k, (g, p) in enumerate(ks):
                look[k // 2][pos][me] += (code(me, g, p) + 1) << (13 * (k % 2))
    item = [[(items[me][w][0] * 32 + items[me][w][1]) if w < nitem[me] else 0 for me in range(NDEV)] for w in range(max(nitem))]
    firsts = [[code(me, own(me)[c], 0) for me in range(NDEV)] for c in (0, 1)]
    sent = []
    for f in range(5):
        lists = [sorted(g for g, fl in fwd[me].items() if f in fl) for me in range(NDEV)]
        for i in range(max(map(len, lists))):
            sent.append((f, [l[i] if i < len(l) else -1 for l in lists]))
    return look, item, firsts, sent


LOOK, ITEM, FIRST, SENT = encode()


def pick(me, row):
    common = max(set(row), key=lambda v: (row.count(v), v))
    out = jnp.int32(common)
    for i, v in enumerate(row):
        if v != common:
            out = jnp.where(me == i, jnp.int32(v), out)
    return out


def entry(values, at):
    if isinstance(at, int):
        return values[at]
    out = values[-1]
    for i, v in enumerate(values[:-1]):
        out = jnp.where(at == i, v, out)
    return out


def rope_tables():
    half = HD // 2
    freq = (np.float32(1.0) / np.power(np.float32(ROPE_BASE), np.arange(half, dtype=np.float32) * np.float32(2.0 / HD))).astype(np.float64)
    sign = np.concatenate([-np.ones(half), np.ones(half)])
    freq = np.concatenate([freq, freq])
    row = np.arange(CHUNK)[:, None] * freq
    base = (np.arange(NCH) * CHUNK)[:, None] * freq
    tabs = np.cos(row), np.sin(row) * sign, np.cos(base), np.sin(base) * sign
    return [t.astype(np.float32) for t in tabs]


def kernel(x_hbm, wq_hbm, wk_hbm, wv_hbm, cr_hbm, sr_hbm, cg_hbm, sg_hbm, o_ref,
           x, wq3, wq, wk, wv, cr, sr, cg, sg, cos, sin, kv, q, flat, s_scr, p_scr, mx_scr, al_scr, m_ref, l_ref, acc, tri,
           in_sem, send_sem, recv_sem):
    me = lax.axis_index('cp')
    core = lax.rem(me, 2)
    y = lax.rem(lax.div(me, 2), 2)

    loads = [(wk_hbm, wk), (wv_hbm, wv), (cr_hbm, cr), (sr_hbm, sr), (cg_hbm, cg), (sg_hbm, sg), (wq_hbm, wq3)]
    loads = [pltpu.make_async_copy(a, b, in_sem.at[i]) for i, (a, b) in enumerate(loads)]

    def load_x(c):
        rows = pl.ds(pl.multiple_of(c * CHUNK, CHUNK), CHUNK)
        return pltpu.make_async_copy(x_hbm.at[rows], x.at[rows], in_sem.at[7 + c])

    for cp in loads[:2] + [load_x(0)] + loads[2:6] + [load_x(1)] + loads[6:]:
        cp.start()

    sib = me + 1 - 2 * core
    mate = me + 2 - 4 * y
    bar = pltpu.get_barrier_semaphore()
    pl.semaphore_signal(bar, inc=1, device_id={'cp': sib}, device_id_type=pl.DeviceIdType.MESH)
    pl.semaphore_signal(bar, inc=1, device_id={'cp': mate}, device_id_type=pl.DeviceIdType.MESH)

    @pl.when(me + 4 < NDEV)
    def _():
        pl.semaphore_signal(bar, inc=1, device_id={'cp': me + 4}, device_id_type=pl.DeviceIdType.MESH)

    @pl.when(me >= 4)
    def _():
        pl.semaphore_signal(bar, inc=1, device_id={'cp': me - 4}, device_id_type=pl.DeviceIdType.MESH)

    looks = [[pick(me, row) for row in word] for word in LOOK]
    item = [pick(me, row) for row in ITEM]
    first = [pick(me, row) for row in FIRST]
    sent = [(f, pick(me, row)) for f, row in SENT]

    def copy_to(piece, f):
        to = (sib, me + 4, me - 4, me + 2, me - 2)[f]
        g, p = lax.div(piece, NP), lax.rem(piece, NP)
        part = kv.at[g, pl.ds(pl.multiple_of(p * CHUNK, CHUNK), CHUNK)]
        return pltpu.make_async_remote_copy(
            src_ref=part, dst_ref=part, send_sem=send_sem.at[f, g], recv_sem=recv_sem.at[piece],
            device_id={'cp': to}, device_id_type=pl.DeviceIdType.MESH)

    def send_on(code, pieces=1):
        piece, flags = lax.rem(code, 64), lax.div(code, 64)
        for f in range(5):
            @pl.when(lax.rem(lax.div(flags, 1 << f), 2) == 1)
            def _():
                for p in range(pieces):
                    copy_to(piece + p, f).start()

    def actions(pos):
        for word in looks:
            packed = entry(word, pos)

            @pl.when(packed > 0)
            def _():
                for k in range(2):
                    code = lax.rem(lax.div(packed, 1 << (13 * k)), 1 << 13) - 1

                    @pl.when((code >= 0) & (code < 2048))
                    def _():
                        copy_to(lax.rem(code, 64), 0).wait_recv()
                        send_on(code)

                    @pl.when(code >= 2048)
                    def _():
                        piece = lax.rem(code, 64)
                        for p in range(NP):
                            copy_to(piece + p, 0).wait_recv()

                        @pl.when(lax.rem(lax.div(code, 64), 2) == 1)
                        def _():
                            for p in range(NP):
                                copy_to(piece + p, 0).start()

    def own_chunk(c):
        return me + c * (NCH - 1 - 2 * me)

    def rope(v, c, rows):
        v = v.astype(jnp.bfloat16).astype(jnp.float32)
        return v * cos[c, rows] + pltpu.roll(v, HD // 2, 1) * sin[c, rows]

    for cp in loads[:6]:
        cp.wait()
    @pl.loop(0, 2)
    def _(c):
        g = own_chunk(c)
        cgr, sgr = cg[pl.ds(g, 1), :], sg[pl.ds(g, 1), :]
        cos[c] = cgr * cr[...] - sgr * sr[...]
        sin[c] = sgr * cr[...] + cgr * sr[...]
        load_x(c).wait()
        wkv = jnp.concatenate([wk[...], wv[...]], axis=1)
        both = jnp.dot(x[pl.ds(pl.multiple_of(c * CHUNK, CHUNK), CHUNK), :], wkv, preferred_element_type=jnp.float32)
        kv[g, pl.ds(0, CHUNK), :] = rope(both[:, :HD], c, slice(0, CHUNK)).astype(jnp.bfloat16)
        for b in range(0, CHUNK, HD):
            kv[g, pl.ds(CHUNK + b, HD), :] = both[b:b + HD, HD:].T.astype(jnp.bfloat16)

        @pl.when(c == 0)
        def _():
            pl.semaphore_wait(bar, 2 + jnp.where(me + 4 < NDEV, 1, 0) + jnp.where(me >= 4, 1, 0))

        send_on(jnp.where(c == 0, first[0], first[1]), NP)

    loads[6].wait()

    @pl.loop(0, DIM // TILE)
    def _(i):
        flat[...] = wq3[pl.ds(pl.multiple_of(i * HEADS * TILE, HEADS * TILE), HEADS * TILE), :].astype(jnp.float32)
        rows = pl.ds(pl.multiple_of(i * TILE, TILE), TILE)
        for h in range(HEADS):
            wq[rows, pl.ds(h * HD, HD)] = flat[pl.ds(h, TILE, stride=HEADS), :].astype(jnp.bfloat16)

    for c in range(2):
        if c == 1:
            actions(0)
        qs = jnp.dot(x[pl.ds(c * CHUNK, CHUNK), :], wq[...], preferred_element_type=jnp.float32)
        for h in range(HEADS):
            for r in range(2):
                rows = slice(r * TILE, (r + 1) * TILE)
                rot = rope(qs[rows, h * HD:(h + 1) * HD], c, rows)
                q[c * NT + h * 2 + r] = (rot * np.float32(HD ** -0.5)).astype(jnp.bfloat16)

    def scores(c, g, t, slot, k0=0, kn=CHUNK, bias=()):
        s = lax.dot_general(kv[g, pl.ds(k0, kn), :], q[c * NT + t], (((1,), (1,)), ((), ())), preferred_element_type=jnp.float32)
        parts = [s] if not bias else [s[i * TILE:(i + 1) * TILE] + b if b is not None else s[i * TILE:(i + 1) * TILE] for i, b in enumerate(bias)]
        tops = []
        for i, part in enumerate(parts):
            rows = part.shape[0]
            s_scr[slot, pl.ds(i * TILE, rows), :] = part
            tops.append(jnp.max(part.reshape(rows // 8, 8, TILE), axis=0))
        mx_scr[slot] = functools.reduce(jnp.maximum, tops)

    def softmax(c, t, slot, kn=CHUNK, first=False):
        n = c * NT + t
        mx = jnp.max(mx_scr[slot], axis=0, keepdims=True)
        if first:
            m_new = mx
        else:
            m_prev = m_ref[n]
            m_new = jnp.maximum(m_prev, mx)
            alpha = jnp.exp(m_prev - m_new)
            al_scr[slot] = alpha
        m_ref[n] = m_new
        p = jnp.exp(s_scr[slot, pl.ds(0, kn), :] - m_new)
        p_scr[slot, pl.ds(0, kn), :] = p.astype(jnp.bfloat16)
        part = jnp.sum(p.reshape(kn // 8, 8, TILE), axis=0)
        l_ref[n] = part if first else l_ref[n] * alpha + part

    def values(c, g, t, slot, k0=0, kn=CHUNK, first=False, last=False):
        vt = jnp.concatenate([kv[g, pl.ds(CHUNK + k0 + b, HD), :] for b in range(0, kn, HD)], axis=1)
        pv = jnp.dot(vt, p_scr[slot, pl.ds(0, kn), :], preferred_element_type=jnp.float32)
        n = c * NT + t
        total = pv if first else acc[n] * al_scr[slot] + pv
        if not last:
            acc[n] = total
            return
        h, r = t // 2, t % 2
        out = total / jnp.sum(l_ref[n], axis=0, keepdims=True)
        o_ref[pl.ds(c * CHUNK + r * TILE, TILE), pl.ds(h * HD, HD)] = out.T.astype(jnp.bfloat16)

    key_i = lax.broadcasted_iota(jnp.int32, (TILE, TILE), 0)
    row_i = lax.broadcasted_iota(jnp.int32, (TILE, TILE), 1)
    none = jnp.where(me < 8, TILE, 0)
    tri[0] = jnp.where(key_i <= row_i, 0.0, -jnp.inf)
    tri[1] = jnp.where(key_i > row_i, 0.0, -jnp.inf)
    tri[2] = jnp.where(key_i > row_i + none, 0.0, -jnp.inf)
    low_far = jnp.where(me < 8, jnp.float32(-jnp.inf), jnp.float32(0.0))

    def edge_blocks(far, then=None):
        def span(i):
            r, low = i % 2, i < NT
            if far:
                edge = tri[2] if low else tri[1]
                return (0, CHUNK, (edge, low_far if low else None)) if r == 0 else (TILE, TILE, (edge,))
            return (0, TILE, (tri[0],)) if r == 0 else (0, CHUNK, (None, tri[0]))

        chunk = [jnp.maximum(own_chunk(c) - 8, 0) if far else own_chunk(c) for c in range(2)]
        for i in range(2 * NT + AHEAD + 1):
            if then is not None and 2 * NT <= i < 2 * NT + AHEAD:
                scores(*then, i - 2 * NT, i % SLOTS)
            if i < 2 * NT:
                scores(i // NT, chunk[i // NT], i % NT, i % SLOTS, *span(i))
            j = i - AHEAD - 1
            if j >= 0:
                values(j // NT, chunk[j // NT], j % NT, j % SLOTS, *span(j)[:2], first=not far, last=far)
            j = i - AHEAD
            if 0 <= j < 2 * NT:
                softmax(j // NT, j % NT, j % SLOTS, span(j)[1], first=not far)

    def c_and_g(code):
        return lax.div(code, 32), lax.rem(code, 32)

    n_full = jnp.minimum(me, 7) + 7
    actions(1)
    edge_blocks(False, then=c_and_g(item[0]))
    p_scr[SLOTS - 1] = jnp.zeros(p_scr.shape[1:], jnp.bfloat16)
    al_scr[SLOTS - 1] = jnp.ones(al_scr.shape[1:], jnp.float32)

    def full_block(w, carry):
        before, now = carry
        actions(w + len(PRE))
        after = jnp.where(w + 1 < n_full, entry(item, w + 1), now)
        c, g = c_and_g(now)
        cn, gn = c_and_g(after)
        cp, gp = c_and_g(before)
        for t in range(NT):
            a = t + AHEAD
            if a < NT:
                scores(c, g, a, a % SLOTS)
            else:
                scores(cn, gn, a - NT, a % SLOTS)
            if t == 0:
                values(cp, gp, NT - 1, SLOTS - 1)
            else:
                values(c, g, t - 1, (t - 1) % SLOTS)
            softmax(c, t, t % SLOTS)
        return now, after

    cl, gl = c_and_g(lax.fori_loop(0, n_full, full_block, (item[0], item[0]))[0])
    actions(n_full + len(PRE))
    values(cl, gl, NT - 1, SLOTS - 1)
    edge_blocks(True)

    for f, g in sent:
        @pl.when(g >= 0)
        def _():
            pltpu.make_async_remote_copy(
                src_ref=kv.at[g], dst_ref=kv.at[g], send_sem=send_sem.at[f, g], recv_sem=recv_sem.at[g * NP],
                device_id={'cp': sib}, device_id_type=pl.DeviceIdType.MESH).wait_send()


def attend(hidden, w_q, w_k, w_v):
    any_spec = pl.BlockSpec(memory_space=pl.ANY)
    f32, bf16 = jnp.float32, jnp.bfloat16
    return pl.pallas_call(
        kernel,
        out_shape=pltpu.VMEM((2 * CHUNK, HEADS * HD), bf16),
        in_specs=[any_spec] * 8,
        out_specs=pl.BlockSpec(memory_space=pltpu.VMEM),
        scratch_shapes=[
            pltpu.VMEM((2 * CHUNK, DIM), bf16),
            pltpu.VMEM((DIM * HEADS, HD), bf16),
            pltpu.VMEM((DIM, HEADS * HD), bf16),
            pltpu.VMEM((DIM, HD), bf16),
            pltpu.VMEM((DIM, HD), bf16),
            pltpu.VMEM((CHUNK, HD), f32),
            pltpu.VMEM((CHUNK, HD), f32),
            pltpu.VMEM((NCH, HD), f32),
            pltpu.VMEM((NCH, HD), f32),
            pltpu.VMEM((2, CHUNK, HD), f32),
            pltpu.VMEM((2, CHUNK, HD), f32),
            pltpu.VMEM((NCH, 2 * CHUNK, HD), bf16),
            pltpu.VMEM((2 * NT, TILE, HD), bf16),
            pltpu.VMEM((HEADS * TILE, HD), f32),
            pltpu.VMEM((SLOTS, CHUNK, TILE), f32),
            pltpu.VMEM((SLOTS, CHUNK, TILE), bf16),
            pltpu.VMEM((SLOTS, 8, TILE), f32),
            pltpu.VMEM((SLOTS, 1, TILE), f32),
            pltpu.VMEM((2 * NT, 1, TILE), f32),
            pltpu.VMEM((2 * NT, 8, TILE), f32),
            pltpu.VMEM((2 * NT, HD, TILE), f32),
            pltpu.VMEM((3, TILE, TILE), f32),
            pltpu.SemaphoreType.DMA((9,)),
            pltpu.SemaphoreType.DMA((5, NCH)),
            pltpu.SemaphoreType.DMA((NCH * NP,)),
        ],
        compiler_params=pltpu.CompilerParams(
            collective_id=0, has_side_effects=True, vmem_limit_bytes=56 << 20),
        cost_estimate=pl.CostEstimate(flops=15 * 10 ** 9, bytes_accessed=16 << 20, transcendentals=1 << 24),
    )(hidden, w_q.reshape(DIM * HEADS, HD), w_k.reshape(DIM, HD), w_v.reshape(DIM, HD), *rope_tables())


def project(heads, w_o):
    rows, cols = 256, 1024
    nr, nc = 2 * CHUNK // rows, DIM // cols

    def body(a, w, out, buf, sem):
        def store(i, j):
            part = pl.ds(i * rows, rows), pl.ds(j * cols, cols)
            return pltpu.make_async_copy(buf.at[part], out.at[part], sem.at[i, j])

        for i in range(nr):
            for j in range(nc):
                y = jnp.dot(a[pl.ds(i * rows, rows), :], w[:, pl.ds(j * cols, cols)], preferred_element_type=jnp.float32)
                buf[pl.ds(i * rows, rows), pl.ds(j * cols, cols)] = y.astype(jnp.bfloat16)
                store(i, j).start()
        for i in range(nr):
            for j in range(nc):
                store(i, j).wait()

    return pl.pallas_call(
        body,
        out_shape=jax.ShapeDtypeStruct((2 * CHUNK, DIM), jnp.bfloat16),
        in_specs=[pl.BlockSpec(memory_space=pltpu.VMEM)] * 2,
        out_specs=pl.BlockSpec(memory_space=pl.ANY),
        scratch_shapes=[pltpu.VMEM((2 * CHUNK, DIM), jnp.bfloat16), pltpu.SemaphoreType.DMA((nr, nc))],
        compiler_params=pltpu.CompilerParams(vmem_limit_bytes=32 << 20),
        cost_estimate=pl.CostEstimate(flops=4 * 2 ** 30, bytes_accessed=13 << 20, transcendentals=0),
    )(heads, pltpu.with_memory_space_constraint(w_o, pltpu.VMEM))


def solution(mesh):
    def device_step(hidden, w_q, w_k, w_v, w_o):
        heads = attend(hidden, w_q, w_k, w_v)
        return project(heads, w_o.reshape(HEADS * HD, DIM))

    from jax.sharding import PartitionSpec as P
    return jax.shard_map(device_step, mesh=mesh, in_specs=(P(('dp', 'cp'), None), P(), P(), P(), P()), out_specs=P(('dp', 'cp'), None), check_vma=False)
```
